32 devices in a mesh: replica: 1 (over z), model2: 4 (over y), model: 8 (over x, core).
Axes of the slice: x: 4, y: 4, z: 1, core: 2. Of those that a mesh axis runs over, the one named last changes fastest.
The devices are a block of a 4x4x8 slice.
Arguments:
- x_prompt: bfloat16 [6, 1, 128, 2048], P('replica')
- lengths: int32 [6, 1], P('replica')
- x_new: bfloat16 [6, 2048], P('replica')
- st_qkv: bfloat16 [8, 2048, 2560], P('model')
- st_out: bfloat16 [8, 2048, 2048], P('model')
- st_gateup: bfloat16 [8, 2048, 11264], P('model')
- st_down_t: bfloat16 [8, 2048, 5632], P('model')
- gain_attn: float32 [8, 2048], replicated
- gain_mlp: float32 [8, 2048], replicated
- tp_query: bfloat16 [8, 2048, 32, 64], P(None, None, ('model', 'model2'))
- tp_key: bfloat16 [8, 2048, 32, 64], P(None, None, ('model', 'model2'))
- tp_value: bfloat16 [8, 2048, 32, 64], P(None, None, ('model', 'model2'))
- tp_out: bfloat16 [8, 32, 64, 2048], P(None, ('model', 'model2'))
- tp_gate: bfloat16 [8, 2048, 5632], P(None, None, ('model', 'model2'))
- tp_up: bfloat16 [8, 2048, 5632], P(None, None, ('model', 'model2'))
- tp_down: bfloat16 [8, 5632, 2048], P(None, ('model', 'model2'))
Outputs:
- output 1: bfloat16 [6, 2048], P('replica')
- output 2: bfloat16 [6, 2048], P('replica')
- output 3: bfloat16 [8, 6, 129, 32, 64], P(None, 'replica', None, ('model', 'model2'))
- output 4: bfloat16 [8, 6, 129, 32, 64], P(None, 'replica', None, ('model', 'model2'))
All inputs are finite; a program needn't handle non-finite values.
Results may differ from the reference program's by a relative error of at most 0.02.
Values are sent between devices in bfloat16 or wider.
A program may use at most 768 MiB of HBM per device.

```python
import jax
import jax.numpy as jnp
from jax import lax

D = 2048
HEADS = 32
KV_HEADS = 4
HEAD = 64
FF = 5632
LAYERS = 8
MICROBATCHES = 6
MICRO_ROWS = 1
BATCH = 6
SEQ_LEN = 128
SLOTS = 32
EPS = 1e-5
THETA = 10000.0


def rms_norm(values_in, gain_vec):
    x_f32 = values_in.astype(jnp.float32)
    inv_rms = lax.rsqrt(jnp.mean(x_f32 * x_f32, axis=-1, keepdims=True) + EPS)
    return (x_f32 * inv_rms * gain_vec).astype(jnp.bfloat16)


def rope_angles(positions):
    half_dim = HEAD // 2
    inv_freq = jnp.power(THETA, jnp.arange(half_dim, dtype=jnp.float32) * (-2.0 / HEAD))
    angles = positions.astype(jnp.float32)[..., None] * inv_freq
    return jnp.cos(angles), jnp.sin(angles)


def apply_rope(values_in, cos_t, sin_t):
    half_dim = values_in.shape[-1] // 2
    first_half = values_in[..., :half_dim]
    second = values_in[..., half_dim:]
    return jnp.concatenate([first_half * cos_t - second * sin_t, second * cos_t + first_half * sin_t], axis=-1)


def draw_lengths(len_key):
    drawn = jax.random.randint(len_key, (BATCH,), SEQ_LEN // 4, SEQ_LEN + 1)
    if BATCH > 1:
        drawn = drawn.at[BATCH - 1].set(SEQ_LEN)
    return drawn.reshape(MICROBATCHES, MICRO_ROWS).astype(jnp.int32)


def setup_inputs(seed: int = 0, part: int = 0) -> dict:
    base_key = jax.random.key(seed)
    shared = jax.random.split(base_key, 7)
    own = jax.random.split(jax.random.fold_in(base_key, part), 4)
    q_cols = HEADS * HEAD
    k_cols = KV_HEADS * HEAD
    w_qkv = (jax.random.normal(shared[0], (LAYERS, D, q_cols + 2 * k_cols), jnp.float32) * D ** -0.5).astype(jnp.bfloat16)
    w_out = (jax.random.normal(shared[1], (LAYERS, q_cols, D), jnp.float32) * q_cols ** -0.5).astype(jnp.bfloat16)
    w_gate = (jax.random.normal(shared[2], (LAYERS, D, FF), jnp.float32) * D ** -0.5).astype(jnp.bfloat16)
    w_up = (jax.random.normal(shared[3], (LAYERS, D, FF), jnp.float32) * D ** -0.5).astype(jnp.bfloat16)
    w_down = (jax.random.normal(shared[4], (LAYERS, FF, D), jnp.float32) * FF ** -0.5).astype(jnp.bfloat16)
    gain_attn = jax.random.uniform(shared[5], (LAYERS, D), jnp.float32, 0.5, 1.5)
    gain_mlp = jax.random.uniform(shared[6], (LAYERS, D), jnp.float32, 0.5, 1.5)
    row_mean = jax.random.normal(own[0], (BATCH, 1, D), jnp.float32)
    x_prompt = (jax.random.normal(own[1], (BATCH, SEQ_LEN, D), jnp.float32) + row_mean).astype(jnp.bfloat16).reshape(MICROBATCHES, MICRO_ROWS, SEQ_LEN, D)
    x_new = jax.random.normal(own[2], (BATCH, D), jnp.float32).astype(jnp.bfloat16)
    lengths = draw_lengths(own[3])
    rep_factor = SLOTS // KV_HEADS
    k_part = w_qkv[:, :, q_cols:q_cols + k_cols].reshape(LAYERS, D, KV_HEADS, HEAD)
    v_part = w_qkv[:, :, q_cols + k_cols:].reshape(LAYERS, D, KV_HEADS, HEAD)
    return {
        'x_prompt': x_prompt,
        'lengths': lengths,
        'x_new': x_new,
        'st_qkv': w_qkv,
        'st_out': w_out,
        'st_gateup': jnp.concatenate([w_gate, w_up], axis=2),
        'st_down_t': jnp.swapaxes(w_down, 1, 2),
        'gain_attn': gain_attn,
        'gain_mlp': gain_mlp,
        'tp_query': w_qkv[:, :, :q_cols].reshape(LAYERS, D, HEADS, HEAD),
        'tp_key': jnp.repeat(k_part, rep_factor, axis=2),
        'tp_value': jnp.repeat(v_part, rep_factor, axis=2),
        'tp_out': w_out.reshape(LAYERS, HEADS, HEAD, D),
        'tp_gate': w_gate,
        'tp_up': w_up,
        'tp_down': w_down,
    }


def prefill_row(x_row, length, st_qkv, st_out, st_gateup, st_down_t, gain_attn, gain_mlp):
    q_cols = HEADS * HEAD
    k_cols = KV_HEADS * HEAD
    group_size = HEADS // KV_HEADS
    positions = jnp.arange(SEQ_LEN)
    cos_t, sin_t = rope_angles(positions)
    key_mask = (positions[None, :] <= positions[:, None]) & (positions[None, :] < length)

    def layer_fn(hidden_x, params):
        g_attn, g_mlp, w_qkv, w_out, w_gateup, w_down_t = params
        normed = rms_norm(hidden_x, g_attn)
        proj_all = jnp.dot(normed, w_qkv, preferred_element_type=jnp.float32)
        queries = apply_rope(proj_all[:, :q_cols].reshape(SEQ_LEN, KV_HEADS, group_size, HEAD), cos_t[:, None, None, :], sin_t[:, None, None, :]).astype(jnp.bfloat16)
        key_rot = apply_rope(proj_all[:, q_cols:q_cols + k_cols].reshape(SEQ_LEN, KV_HEADS, HEAD), cos_t[:, None, :], sin_t[:, None, :]).astype(jnp.bfloat16)
        val_proj = proj_all[:, q_cols + k_cols:].reshape(SEQ_LEN, KV_HEADS, HEAD).astype(jnp.bfloat16)
        scores = jnp.einsum('qcge,kce->cgqk', queries.astype(jnp.float32), key_rot.astype(jnp.float32)) * HEAD ** -0.5
        scores = jnp.where(key_mask, scores, -1e30)
        probs_bf = jax.nn.softmax(scores, axis=-1).astype(jnp.bfloat16)
        attn_out = jnp.einsum('cgqk,kce->qcge', probs_bf.astype(jnp.float32), val_proj.astype(jnp.float32)).astype(jnp.bfloat16).reshape(SEQ_LEN, q_cols)
        resid_mid = (hidden_x.astype(jnp.float32) + jnp.dot(attn_out, w_out, preferred_element_type=jnp.float32)).astype(jnp.bfloat16)
        normed_mlp = rms_norm(resid_mid, g_mlp)
        gate_up = jnp.dot(normed_mlp, w_gateup, preferred_element_type=jnp.float32)
        act_out = (jax.nn.silu(gate_up[:, :FF]) * gate_up[:, FF:]).astype(jnp.bfloat16)
        layer_out = (resid_mid.astype(jnp.float32) + jnp.dot(act_out, w_down_t.T, preferred_element_type=jnp.float32)).astype(jnp.bfloat16)
        return layer_out, (key_rot, val_proj)

    final_x, kv_pair = lax.scan(layer_fn, x_row, (gain_attn, gain_mlp, st_qkv, st_out, st_gateup, st_down_t))
    last_row = lax.dynamic_index_in_dim(final_x, length - 1, axis=0, keepdims=False)
    return last_row, kv_pair[0], kv_pair[1]


def reference(x_prompt, lengths, x_new, st_qkv, st_out, st_gateup, st_down_t, gain_attn, gain_mlp, tp_query, tp_key, tp_value, tp_out, tp_gate, tp_up, tp_down):
    rows_x = x_prompt.reshape(BATCH, SEQ_LEN, D)
    len_flat = lengths.reshape(BATCH)
    last_hidden, k_rows, v_rows = lax.map(lambda row_pair: prefill_row(row_pair[0], row_pair[1], st_qkv, st_out, st_gateup, st_down_t, gain_attn, gain_mlp), (rows_x, len_flat))
    rep_factor = SLOTS // KV_HEADS
    k_cache = jnp.repeat(jnp.swapaxes(k_rows, 0, 1), rep_factor, axis=3)
    v_cache = jnp.repeat(jnp.swapaxes(v_rows, 0, 1), rep_factor, axis=3)
    group_slot = HEADS // SLOTS
    cos_n, sin_n = rope_angles(len_flat)
    cached = jnp.arange(SEQ_LEN)[None, :] < len_flat[:, None]
    score_scale = HEAD ** -0.5

    def dec_layer(hidden_x, params):
        g_attn, g_mlp, w_query, w_key, w_value, w_outp, w_gate, w_upp, w_down, k_cached, v_cached = params
        normed = rms_norm(hidden_x, g_attn)
        normed_f = normed.astype(jnp.float32)
        queries = apply_rope(jnp.einsum('bd,dhe->bhe', normed_f, w_query.astype(jnp.float32)), cos_n[:, None, :], sin_n[:, None, :])
        queries = queries.astype(jnp.bfloat16).reshape(BATCH, SLOTS, group_slot, HEAD).astype(jnp.float32)
        key_new = apply_rope(jnp.einsum('bd,dce->bce', normed_f, w_key.astype(jnp.float32)), cos_n[:, None, :], sin_n[:, None, :]).astype(jnp.bfloat16)
        val_new = jnp.einsum('bd,dce->bce', normed_f, w_value.astype(jnp.float32)).astype(jnp.bfloat16)
        s_old = jnp.einsum('bcge,bsce->bcgs', queries, k_cached.astype(jnp.float32)) * score_scale
        s_old = jnp.where(cached[:, None, None, :], s_old, -1e30)
        s_new = jnp.einsum('bcge,bce->bcg', queries, key_new.astype(jnp.float32)) * score_scale
        row_max = jnp.maximum(jnp.max(s_old, axis=-1), s_new)
        e_old = jnp.exp(s_old - row_max[..., None])
        e_new = jnp.exp(s_new - row_max)
        denom_sum = jnp.sum(e_old, axis=-1) + e_new
        p_old = (e_old / denom_sum[..., None]).astype(jnp.bfloat16)
        p_new = (e_new / denom_sum).astype(jnp.bfloat16)
        attn_out = jnp.einsum('bcgs,bsce->bcge', p_old.astype(jnp.float32), v_cached.astype(jnp.float32)) + p_new.astype(jnp.float32)[..., None] * val_new.astype(jnp.float32)[:, :, None, :]
        attn_out = attn_out.astype(jnp.bfloat16).reshape(BATCH, HEADS, HEAD)
        resid_mid = (hidden_x.astype(jnp.float32) + jnp.einsum('bhe,hed->bd', attn_out.astype(jnp.float32), w_outp.astype(jnp.float32))).astype(jnp.bfloat16)
        normed_mlp = rms_norm(resid_mid, g_mlp)
        act_out = (jax.nn.silu(jnp.dot(normed_mlp, w_gate, preferred_element_type=jnp.float32)) * jnp.dot(normed_mlp, w_upp, preferred_element_type=jnp.float32)).astype(jnp.bfloat16)
        layer_out = (resid_mid.astype(jnp.float32) + jnp.dot(act_out, w_down, preferred_element_type=jnp.float32)).astype(jnp.bfloat16)
        return layer_out, (key_new, val_new)

    dec_out, new_kv = lax.scan(dec_layer, x_new, (gain_attn, gain_mlp, tp_query, tp_key, tp_value, tp_out, tp_gate, tp_up, tp_down, k_cache, v_cache))
    k_full = jnp.concatenate([k_cache, new_kv[0][:, :, None]], axis=2)
    v_full = jnp.concatenate([v_cache, new_kv[1][:, :, None]], axis=2)
    return (dec_out, last_hidden, k_full, v_full)
```

```python
import functools

import jax
import jax.numpy as jnp
from jax import lax
from jax.experimental import pallas as pl
from jax.experimental.pallas import tpu as pltpu
from jax.sharding import PartitionSpec as P

EPS = 1e-5
THETA = 10000.0
TP_AXES = ('model', 'model2')
MESH = pl.DeviceIdType.MESH
BLK = 256
LANES = 128
NSLOT = 50
NEG = -1e30


def rope_angles(positions, head_dim):
    half_dim = head_dim // 2
    inv_freq = jnp.power(THETA, jnp.arange(half_dim, dtype=jnp.float32) * (-2.0 / head_dim))
    angles = positions.astype(jnp.float32)[..., None] * inv_freq
    return jnp.cos(angles), jnp.sin(angles)


def dot_nn(a, b):
    return lax.dot_general(a, b, (((1,), (0,)), ((), ())), preferred_element_type=jnp.float32)


def dot_nt(a, b):
    return lax.dot_general(a, b, (((1,), (1,)), ((), ())), preferred_element_type=jnp.float32)


def stage_kernel(dims, x_hbm, dec_hbm, cos_ref, sin_ref, mask_a_ref, mask_b_ref, sel_ref, ga_ref, gm_ref,
                 w_qkv, w_out, w_gu, w_dt, kv_out, res_out,
                 ring, xin, xout, hbuf, qbuf, x1buf, abuf, kvp, kva, kvb, kv_recv, res_vm,
                 ring_sem, x0_sem, xs_sem, xr_sem, ks_sem, kr_sem, rs_sem, rr_sem, pair_sem):
    stages, width, kv_heads, head_dim, seq_a, seq_b, n_dec, q_cols, ff = dims
    n_rows = seq_a + n_dec + seq_b
    row_b = seq_a + n_dec
    d_model = w_out.shape[2]
    nx = d_model // BLK
    nq = q_cols // BLK
    nff = ff // BLK
    n_dev = stages * width
    per_head = stages // kv_heads
    stage = lax.axis_index('model')
    col = lax.axis_index('model2')
    me = stage * width + col
    half = lax.rem(col, 2)

    def ring_copy(src, slot):
        return pltpu.make_async_copy(src, ring.at[slot], ring_sem.at[slot])

    def cols(ref, c):
        return ref.at[0, :, pl.ds(pl.multiple_of(c * BLK, BLK), BLK)]

    def wait_slot(slot):
        ring_copy(cols(w_out, 0), slot).wait()

    order = [(w_qkv, nq), (w_qkv, nq + 1)] + [(w_qkv, c) for c in range(nq)] + [(w_out, c) for c in range(nx)]
    n_attn = len(order)
    for j in range(nff):
        order += [(w_gu, j), (w_gu, nff + j)]
    n_up = len(order)
    order += [(w_dt, c) for c in range(nff)]

    def issue(i):
        ref, c = order[i]
        ring_copy(cols(ref, c), i % NSLOT).start()

    for i in range(NSLOT):
        issue(i)

    barrier = pltpu.get_barrier_semaphore()

    def greet(d, carry):
        @pl.when(d != me)
        def _():
            pl.semaphore_signal(barrier, inc=1, device_id={'model': d // width, 'model2': lax.rem(d, width)}, device_id_type=MESH)
        return carry

    lax.fori_loop(0, n_dev, greet, 0)
    pl.semaphore_wait(barrier, n_dev - 1)

    @pl.when(stage == 0)
    def _():
        copies = []
        for n in range(nx):
            cs = pl.ds(n * BLK, BLK)
            copies.append(pltpu.make_async_copy(x_hbm.at[col, 0, :, cs], xin.at[n, pl.ds(0, seq_a), :], x0_sem.at[3 * n]))
            copies.append(pltpu.make_async_copy(dec_hbm.at[:, cs], xin.at[n, pl.ds(seq_a, n_dec), :], x0_sem.at[3 * n + 1]))
            copies.append(pltpu.make_async_copy(x_hbm.at[width + col // 2, 0, pl.ds(pl.multiple_of(half * seq_b, seq_b), seq_b), cs], xin.at[n, pl.ds(row_b, seq_b), :], x0_sem.at[3 * n + 2]))
        for c in copies:
            c.start()
        for c in copies:
            c.wait()

    def x_send(n):
        return pltpu.make_async_remote_copy(src_ref=xout.at[n], dst_ref=xin.at[n], send_sem=xs_sem.at[n], recv_sem=xr_sem.at[n],
                                            device_id={'model': lax.rem(stage + 1, stages), 'model2': col}, device_id_type=MESH)

    @pl.when(stage > 0)
    def _():
        for n in range(nx):
            x_send(n).wait_recv()

    def rms_into(src, gain_ref):
        ss = jnp.zeros((n_rows, 1), jnp.float32)
        for n in range(nx):
            v = src[n].astype(jnp.float32)
            ss = ss + jnp.sum(v * v, axis=-1, keepdims=True)
        inv = lax.rsqrt(ss * (1.0 / d_model) + EPS)
        for n in range(nx):
            g = gain_ref[pl.ds(stage, 1), n * BLK:(n + 1) * BLK]
            hbuf[:, n * BLK:(n + 1) * BLK] = (src[n].astype(jnp.float32) * inv * g).astype(jnp.bfloat16)

    rms_into(xin, ga_ref)

    lane = lax.broadcasted_iota(jnp.int32, (n_rows, LANES), 1)
    first_half = lax.rem(lane, head_dim) < head_dim // 2
    low = lane < head_dim

    def rope(y):
        swapped = jnp.where(first_half, pltpu.roll(y, LANES - head_dim // 2, 1), pltpu.roll(y, head_dim // 2, 1))
        return y * cos_ref[...] + swapped * sin_ref[...]

    wait_slot(0)
    wait_slot(1)
    k_all = dot_nn(hbuf[...], ring[0])
    v_all = dot_nn(hbuf[...], ring[1])
    for c in range(kv_heads):
        p = c // 2
        kk = rope(k_all[:, p * LANES:(p + 1) * LANES])
        vv = v_all[:, p * LANES:(p + 1) * LANES]
        if c % 2 == 0:
            packed = jnp.where(low, kk, pltpu.roll(vv, head_dim, 1))
        else:
            packed = jnp.where(low, pltpu.roll(kk, head_dim, 1), vv)
        kvp[c] = packed.astype(jnp.bfloat16)

    def pair_copy():
        return pltpu.make_async_remote_copy(src_ref=kvp.at[:, pl.ds(row_b, seq_b), :], dst_ref=kv_recv, send_sem=pair_sem.at[0], recv_sem=pair_sem.at[1],
                                            device_id={'model': stage, 'model2': col + 1 - 2 * half}, device_id_type=MESH)

    @pl.when(half == 0)
    def _():
        pair_copy().start()

    def q_step(c, carry):
        wait_slot(2 + 2 * c)
        wait_slot(3 + 2 * c)
        h = hbuf[...]
        qs = [dot_nn(h, ring[2 + 2 * c]), dot_nn(h, ring[3 + 2 * c])]
        for t in range(2):
            for p in range(2):
                start = pl.multiple_of((2 * c + t) * BLK + p * LANES, LANES)
                qbuf[:, pl.ds(start, LANES)] = rope(qs[t][:, p * LANES:(p + 1) * LANES]).astype(jnp.bfloat16)
        return carry

    lax.fori_loop(0, nq // 2, q_step, 0)
    for i in range(NSLOT, NSLOT + nq + 2):
        issue(i)

    def kv_copy(d, src_stage, src_col):
        return pltpu.make_async_remote_copy(src_ref=kvp.at[d // (per_head * width)], dst_ref=kv_out.at[src_stage, src_col], send_sem=ks_sem.at[d],
                                            recv_sem=kr_sem.at[src_stage * width + src_col],
                                            device_id={'model': d // width, 'model2': lax.rem(d, width)}, device_id_type=MESH)

    def kv_local():
        return pltpu.make_async_copy(kvp.at[stage // per_head], kv_out.at[stage, col], ks_sem.at[me])

    def kv_start(d, carry):
        @pl.when(d != me)
        def _():
            kv_copy(d, stage, col).start()
        return carry

    lax.fori_loop(0, n_dev, kv_start, 0)
    kv_local().start()

    @pl.when(half == 1)
    def _():
        pair_copy().wait_recv()

    low_s = lax.broadcasted_iota(jnp.int32, (seq_a, LANES), 1) < head_dim
    for c in range(kv_heads):
        own_b = kvp[c, row_b:row_b + seq_b, :]

        @pl.when(half == 0)
        def _():
            kvb[c, 0, 0:seq_b, :] = own_b

        @pl.when(half == 1)
        def _():
            kvb[c, 0, 0:seq_b, :] = kv_recv[c]

        kvb[c, 0, seq_b:2 * seq_b, :] = own_b
        for src, dst in ((kvp[c, 0:seq_a, :], kva), (kvb[c, 0, 0:seq_a, :], kvb)):
            f = src.astype(jnp.float32)
            r = pltpu.roll(f, head_dim, 1)
            dst[c, 1, 0:seq_a, :] = jnp.where(low_s, f, 0.0).astype(jnp.bfloat16)
            dst[c, 1, seq_a:2 * seq_a, :] = jnp.where(low_s, 0.0, r).astype(jnp.bfloat16)
            dst[c, 2, 0:seq_a, :] = jnp.where(low_s, r, 0.0).astype(jnp.bfloat16)
            dst[c, 2, seq_a:2 * seq_a, :] = jnp.where(low_s, 0.0, f).astype(jnp.bfloat16)

    scale = head_dim ** -0.5
    mask_a = mask_a_ref[...] > 0
    mask_b = mask_b_ref[...] > 0
    mask_da = mask_a[seq_a:, :]
    mask_db = mask_b[:n_dec, :]
    low_d = lax.broadcasted_iota(jnp.int32, (n_dec, LANES), 1) < head_dim
    row_d = lax.broadcasted_iota(jnp.int32, (n_dec, LANES), 0)

    def soft(s, mask):
        s = jnp.where(mask, s * scale, NEG)
        m = jnp.max(s, axis=-1, keepdims=True)
        e = jnp.exp(s - m)
        return (e * (1.0 / jnp.sum(e, axis=-1, keepdims=True))).astype(jnp.bfloat16)

    def soft_self(s, mask, s_self):
        s = jnp.where(mask, s * scale, NEG)
        m = jnp.maximum(jnp.max(s, axis=-1, keepdims=True), s_self)
        e = jnp.exp(s - m)
        e_self = jnp.exp(s_self - m)
        inv = 1.0 / (jnp.sum(e, axis=-1, keepdims=True) + e_self)
        return (e * inv).astype(jnp.bfloat16), (e_self * inv).astype(jnp.bfloat16).astype(jnp.float32)

    pairs_per_kv = q_cols // (kv_heads * LANES)
    for c in range(kv_heads):
        kv_d = kvp[c, seq_a:seq_a + n_dec, :].astype(jnp.float32)
        kv_r = pltpu.roll(kv_d, head_dim, 1)
        k_self = jnp.where(low_d, kv_d, kv_r)
        v_self = jnp.where(low_d, kv_r, kv_d)

        def head_pair(t, carry, c=c, k_self=k_self, v_self=v_self):
            hs = pl.ds(pl.multiple_of((c * pairs_per_kv + t) * LANES, LANES), LANES)
            qd = qbuf[seq_a:row_b, hs].astype(jnp.float32)
            prod = qd * k_self
            self_e = jnp.sum(jnp.where(low_d, prod, 0.0), axis=-1, keepdims=True) * scale
            self_o = jnp.sum(jnp.where(low_d, 0.0, prod), axis=-1, keepdims=True) * scale
            s_a = dot_nt(qbuf[0:row_b, hs], kva[c, 1])
            s_b = dot_nt(qbuf[seq_a:n_rows, hs], kvb[c, 1])
            pa = jnp.concatenate([soft(s_a[:seq_a, :seq_a], mask_a[:seq_a]), soft(s_a[:seq_a, seq_a:], mask_a[:seq_a])], axis=1)
            pb = jnp.concatenate([soft(s_b[n_dec:, :seq_a], mask_b[n_dec:]), soft(s_b[n_dec:, seq_a:], mask_b[n_dec:])], axis=1)
            dae, dae_s = soft_self(s_a[seq_a:, :seq_a], mask_da, self_e)
            dao, dao_s = soft_self(s_a[seq_a:, seq_a:], mask_da, self_o)
            dbe, dbe_s = soft_self(s_b[:n_dec, :seq_a], mask_db, self_e)
            dbo, dbo_s = soft_self(s_b[:n_dec, seq_a:], mask_db, self_o)
            o_a = dot_nn(jnp.concatenate([pa, jnp.concatenate([dae, dao], axis=1)], axis=0), kva[c, 2])
            o_b = dot_nn(jnp.concatenate([jnp.concatenate([dbe, dbo], axis=1), pb], axis=0), kvb[c, 2])
            o_da = o_a[seq_a:] + jnp.where(low_d, dae_s, dao_s) * v_self
            o_db = o_b[:n_dec] + jnp.where(low_d, dbe_s, dbo_s) * v_self
            hbuf[0:seq_a, hs] = o_a[:seq_a].astype(jnp.bfloat16)
            hbuf[seq_a:row_b, hs] = jnp.where(row_d == 0, o_da, o_db).astype(jnp.bfloat16)
            hbuf[row_b:n_rows, hs] = o_b[n_dec:].astype(jnp.bfloat16)
            return carry

        lax.fori_loop(0, pairs_per_kv, head_pair, 0)

    def out_step(n, carry):
        s0 = nq + 2 + 2 * n
        wait_slot(s0)
        wait_slot(s0 + 1)
        o = hbuf[...]
        y0 = dot_nn(o, ring[s0])
        y1 = dot_nn(o, ring[s0 + 1])
        x1buf[2 * n] = (xin[2 * n].astype(jnp.float32) + y0).astype(jnp.bfloat16)
        x1buf[2 * n + 1] = (xin[2 * n + 1].astype(jnp.float32) + y1).astype(jnp.bfloat16)
        return carry

    lax.fori_loop(0, nx // 2, out_step, 0)
    for i in range(NSLOT + nq + 2, NSLOT + n_attn):
        issue(i)

    rms_into(x1buf, gm_ref)

    n_tail = len(order) - (NSLOT + n_attn)

    def gu_step(j, carry):
        i0 = n_attn + 2 * j
        sg = lax.rem(i0, NSLOT)
        su = lax.rem(i0 + 1, NSLOT)
        wait_slot(sg)
        wait_slot(su)
        h = hbuf[...]
        g = dot_nn(h, ring[sg])
        u = dot_nn(h, ring[su])
        abuf[j] = (g * (1.0 / (1.0 + jnp.exp(-g))) * u).astype(jnp.bfloat16)

        @pl.when(j < n_tail // 2)
        def _():
            c0 = NSLOT + n_attn - n_up + 2 * j
            ring_copy(cols(w_dt, c0), sg).start()
            ring_copy(cols(w_dt, c0 + 1), su).start()
        return carry

    lax.fori_loop(0, nff, gu_step, 0)

    d_slots = [(n_up + k) % NSLOT for k in range(nff)]
    for s in d_slots:
        wait_slot(s)

    def down_step(n, carry):
        ys = []
        for t in range(2):
            rows = pl.ds(pl.multiple_of((2 * n + t) * BLK, BLK), BLK)
            acc = dot_nt(abuf[0], ring[d_slots[0], rows, :])
            for k in range(1, nff):
                acc = acc + dot_nt(abuf[k], ring[d_slots[k], rows, :])
            ys.append(acc)
        for t in range(2):
            xout[2 * n + t] = (x1buf[2 * n + t].astype(jnp.float32) + ys[t]).astype(jnp.bfloat16)

        @pl.when(stage < stages - 1)
        def _():
            x_send(2 * n).start()
            x_send(2 * n + 1).start()
        return carry

    lax.fori_loop(0, nx // 2, down_step, 0)

    def res_copy(d, src_col):
        return pltpu.make_async_remote_copy(src_ref=res_vm, dst_ref=res_out.at[src_col], send_sem=rs_sem.at[d], recv_sem=rr_sem.at[src_col],
                                            device_id={'model': d // width, 'model2': lax.rem(d, width)}, device_id_type=MESH)

    def res_local():
        return pltpu.make_async_copy(res_vm, res_out.at[col], rs_sem.at[me])

    groups = n_dec // 4
    last = stages - 1

    @pl.when(stage == last)
    def _():
        for j in range(nx // groups):
            acc = dot_nn(sel_ref[0], xout[groups * j])
            for i in range(1, groups):
                acc = acc + dot_nn(sel_ref[i], xout[groups * j + i])
            res_vm[:, j * BLK:(j + 1) * BLK] = acc.astype(jnp.bfloat16)

        def res_start(d, carry):
            @pl.when(d != me)
            def _():
                res_copy(d, col).start()
            return carry

        lax.fori_loop(0, n_dev, res_start, 0)
        res_local().start()

        def res_wait(d, carry):
            @pl.when(d != me)
            def _():
                res_copy(d, col).wait_send()
            return carry

        lax.fori_loop(0, n_dev, res_wait, 0)
        res_local().wait()

    @pl.when(stage < last)
    def _():
        for n in range(nx):
            x_send(n).wait_send()

    @pl.when(half == 0)
    def _():
        pair_copy().wait_send()

    kv_local().wait()

    def kv_wait(d, carry):
        @pl.when(d != me)
        def _():
            kv_copy(d, stage, col).wait_send()
            kv_copy(0, d // width, lax.rem(d, width)).wait_recv()
        return carry

    lax.fori_loop(0, n_dev, kv_wait, 0)

    def res_in(y, carry):
        @pl.when((stage != last) | (y != col))
        def _():
            res_copy(0, y).wait_recv()
        return carry

    lax.fori_loop(0, width, res_in, 0)


def solution(mesh):
    stages = mesh.shape['model']
    width = mesh.shape['model2']
    stage_spec = P('model', None, None)
    in_specs = (P('replica', None, None, None), P('replica', None), P('replica', None),
                stage_spec, stage_spec, stage_spec, stage_spec, P(None, None), P(None, None),
                P(None, None, TP_AXES, None), P(None, None, TP_AXES, None), P(None, None, TP_AXES, None),
                P(None, TP_AXES, None, None), P(None, None, TP_AXES), P(None, None, TP_AXES), P(None, TP_AXES, None))
    cache_spec = P(None, 'replica', None, TP_AXES, None)
    out_specs = (P('replica', None), P('replica', None), cache_spec, cache_spec)

    def shard_body(x_prompt, lengths, x_new, st_qkv, st_out, st_gateup, st_down_t, gain_attn, gain_mlp, tp_query, tp_key, tp_value, tp_out, tp_gate, tp_up, tp_down):
        n_prompts, _, seq_len, d_model = x_prompt.shape
        head_dim = tp_query.shape[-1]
        q_cols = st_out.shape[1]
        kv_heads = (st_qkv.shape[2] - q_cols) // (2 * head_dim)
        ff = st_down_t.shape[2]
        n_dec = 16
        seq_a, seq_b = seq_len, seq_len // 2
        assert n_prompts == width + width // 2 and st_qkv.shape[0] == 1 and tp_key.shape[2] == 1
        n_rows = seq_a + n_dec + seq_b
        groups = n_dec // 4
        col = lax.axis_index('model2')
        half = col % 2
        lens = lengths.reshape(n_prompts)
        ib = width + col // 2
        len_a, len_b = lens[col], lens[ib]
        bf = jnp.bfloat16
        xa, xb = x_new[col], jnp.where(half == 1, x_new[ib], jnp.zeros((d_model,), bf))
        dec_rows = jnp.concatenate([xa[None], xb[None], jnp.zeros((n_dec - 2, d_model), bf)], axis=0)
        ar = jnp.arange(n_rows)
        pos = jnp.where(ar < seq_a, ar, jnp.where(ar == seq_a, len_a, jnp.where(ar == seq_a + 1, len_b, half * seq_b + ar - seq_a - n_dec)))
        cos_t, sin_t = rope_angles(pos, head_dim)
        cos_w = jnp.concatenate([cos_t] * (2 * LANES // head_dim), axis=1)
        sin_w = jnp.concatenate([-sin_t, sin_t] * (LANES // head_dim), axis=1)
        is_dec = (ar >= seq_a) & (ar < seq_a + n_dec)
        key_pos = jnp.arange(seq_len)[None, :]
        seen = is_dec[:, None] | (key_pos <= pos[:, None])
        mask_a = (seen & (key_pos < len_a))[:seq_a + n_dec].astype(jnp.float32)
        mask_b = (seen & (key_pos < len_b))[seq_a:].astype(jnp.float32)
        off_b = len_b - 1 - half * seq_b
        pick = jnp.stack([len_a - 1, jnp.where((off_b >= 0) & (off_b < seq_b), seq_a + n_dec + off_b, -1), jnp.full((), seq_a), jnp.where(half == 1, seq_a + 1, -1)])
        onehot = (pick[:, None] == ar[None, :]).astype(bf)
        eye = jnp.eye(groups, dtype=bf)
        sel = (eye[:, :, None, None] * onehot[None, None]).reshape(groups, n_dec, n_rows)

        dims = (stages, width, kv_heads, head_dim, seq_a, seq_b, n_dec, q_cols, ff)
        nx = d_model // BLK
        n_dev = stages * width
        vmem, hbm = pl.BlockSpec(memory_space=pltpu.VMEM), pl.BlockSpec(memory_space=pl.ANY)
        dma = pltpu.SemaphoreType.DMA
        kv_all, res = pl.pallas_call(
            functools.partial(stage_kernel, dims),
            out_shape=(jax.ShapeDtypeStruct((stages, width, n_rows, LANES), bf), jax.ShapeDtypeStruct((width, n_dec, d_model // groups), bf)),
            in_specs=[hbm, hbm] + [vmem] * 7 + [hbm] * 4,
            out_specs=(hbm, hbm),
            scratch_shapes=[
                pltpu.VMEM((NSLOT, d_model, BLK), bf),
                pltpu.VMEM((nx, n_rows, BLK), bf),
                pltpu.VMEM((nx, n_rows, BLK), bf),
                pltpu.VMEM((n_rows, d_model), bf),
                pltpu.VMEM((n_rows, q_cols), bf),
                pltpu.VMEM((nx, n_rows, BLK), bf),
                pltpu.VMEM((ff // BLK, n_rows, BLK), bf),
                pltpu.VMEM((kv_heads, n_rows, LANES), bf),
                pltpu.VMEM((kv_heads, 3, 2 * seq_a, LANES), bf),
                pltpu.VMEM((kv_heads, 3, 2 * seq_a, LANES), bf),
                pltpu.VMEM((kv_heads, seq_b, LANES), bf),
                pltpu.VMEM((n_dec, d_model // groups), bf),
                dma((NSLOT,)), dma((3 * nx,)), dma((nx,)), dma((nx,)), dma((n_dev,)), dma((n_dev,)), dma((n_dev,)), dma((width,)), dma((2,)),
            ],
            compiler_params=pltpu.CompilerParams(collective_id=0, has_side_effects=True, vmem_limit_bytes=67043328),
        )(x_prompt, dec_rows, cos_w, sin_w, mask_a, mask_b, sel, gain_attn, gain_mlp, st_qkv, st_out, st_gateup, st_down_t)

        picked = res.reshape(width, groups, 4, nx // groups, BLK).transpose(0, 2, 3, 1, 4).reshape(width, 4, d_model)
        last_hidden = jnp.concatenate([picked[:, 0], picked[0::2, 1] + picked[1::2, 1]], axis=0)
        dec_out = jnp.concatenate([picked[:, 2], picked[1::2, 3]], axis=0)

        def cache(part):
            sub = kv_all[..., part * head_dim:(part + 1) * head_dim]
            own = sub[:, :, :seq_a + 1]
            lo, hi = sub[:, 0::2, seq_a + n_dec:], sub[:, 1::2, seq_a + n_dec:]
            shared = jnp.concatenate([lo, hi, sub[:, 1::2, seq_a + 1:seq_a + 2]], axis=2)
            return jnp.concatenate([own, shared], axis=1)[:, :, :, None, :]

        return dec_out, last_hidden, cache(0), cache(1)

    return jax.shard_map(shard_body, mesh=mesh, in_specs=in_specs, out_specs=out_specs, check_vma=False)
```

```python
import functools

import jax
import jax.numpy as jnp
import numpy as np
from jax import lax
from jax.experimental import pallas as pl
from jax.experimental.pallas import tpu as pltpu
from jax.sharding import PartitionSpec as P

EPS = 1e-5
THETA = 10000.0
TP_AXES = ('model', 'model2')
MESH = pl.DeviceIdType.MESH
BLK = 256
LANES = 128
NSLOT = 50
NEG = -1e30
QU = 4
GU = 4


def rope_table(count, head_dim):
    half_dim = head_dim // 2
    inv_freq = np.power(np.float32(THETA), np.arange(half_dim, dtype=np.float32) * np.float32(-2.0 / head_dim))
    angles = (np.arange(count, dtype=np.float32)[:, None] * inv_freq.astype(np.float32)).astype(np.float64)
    cos, sin = np.cos(angles).astype(np.float32), np.sin(angles).astype(np.float32)
    return jnp.asarray(np.tile(cos, (1, 2 * LANES // head_dim))), jnp.asarray(np.tile(np.concatenate([-sin, sin], axis=1), (1, LANES // head_dim)))


def dot_nn(a, b):
    return lax.dot_general(a, b, (((1,), (0,)), ((), ())), preferred_element_type=jnp.float32)


def dot_nt(a, b):
    return lax.dot_general(a, b, (((1,), (1,)), ((), ())), preferred_element_type=jnp.float32)


def cat(ref, first, count):
    return jnp.concatenate([ref[first + t] for t in range(count)], axis=1)


def stage_kernel(dims, lens_ref, cos_t, sin_t, ga_ref, gm_ref, new_ref, x_hbm, w_qkv, w_out, w_gu, w_dt, kv_out, dec_out, res_out,
                 ring, xin, xout, hbuf, qbuf, x1buf, abuf, kvp, kva, kvb, kv_recv, kvt, cosv, sinv, gains, mask_a, mask_b, res_vm, small, asmall, tsmall,
                 ring_sem, x0_sem, xs_sem, xr_sem, ks_sem, kr_sem, kd_sem, rs_sem, rr_sem, pair_sem):
    stages, width, kv_heads, head_dim, seq_a, seq_b, n_dec, q_cols, ff, n_prompts = dims
    n_rows = seq_a + n_dec + seq_b
    row_b = seq_a + n_dec
    d_model = w_out.shape[2]
    nx = d_model // BLK
    nl = d_model // LANES
    nq = q_cols // BLK
    nff = ff // BLK
    n_dev = stages * width
    per_head = stages // kv_heads
    last = stages - 1
    bf, f32 = jnp.bfloat16, jnp.float32
    stage = lax.axis_index('model')
    col = lax.axis_index('model2')
    me = stage * width + col
    half = lax.rem(col, 2)
    shared = width + col // 2
    len_a = lens_ref[col, 0]
    len_b = lens_ref[shared, 0]

    def ring_copy(ref, c, slot, t):
        start = pl.multiple_of(c * BLK + t * LANES, LANES)
        return pltpu.make_async_copy(ref.at[0, :, pl.ds(start, LANES)], ring.at[2 * slot + t], ring_sem.at[2 * slot + t])

    def ring_start(ref, c, slot):
        ring_copy(ref, c, slot, 0).start()
        ring_copy(ref, c, slot, 1).start()

    def wait_slot(slot):
        ring_copy(w_out, 0, slot, 0).wait()
        ring_copy(w_out, 0, slot, 1).wait()

    def weight(slot):
        return cat(ring, 2 * slot, 2)

    order = [(w_qkv, nq), (w_qkv, nq + 1)] + [(w_qkv, c) for c in range(nq)] + [(w_out, c) for c in range(nx)]
    n_attn = len(order)
    for j in range(nff):
        order += [(w_gu, j), (w_gu, nff + j)]
    n_up = len(order)
    order += [(w_dt, c) for c in range(nff)]

    def issue(i):
        ref, c = order[i]
        ring_start(ref, c, i % NSLOT)

    def x0_copies():
        out = []
        for n in range(nl):
            cs = pl.ds(n * LANES, LANES)
            out.append(pltpu.make_async_copy(x_hbm.at[col, 0, :, cs], xin.at[n, pl.ds(0, seq_a), :], x0_sem.at[2 * n]))
            out.append(pltpu.make_async_copy(x_hbm.at[shared, 0, pl.ds(pl.multiple_of(half * seq_b, seq_b), seq_b), cs], xin.at[n, pl.ds(row_b, seq_b), :], x0_sem.at[2 * n + 1]))
        return out

    @pl.when(stage == 0)
    def _():
        for c in x0_copies():
            c.start()

    for i in range(NSLOT):
        issue(i)

    barrier = pltpu.get_barrier_semaphore()

    def device(d):
        return {'model': d // width, 'model2': lax.rem(d, width)}

    def greet(i, carry):
        pl.semaphore_signal(barrier, inc=1, device_id=device(lax.rem(me + i, n_dev)), device_id_type=MESH)
        return carry

    lax.fori_loop(1, n_dev, greet, 0)

    for which, ref in ((0, ga_ref), (1, gm_ref)):
        mine = lax.broadcasted_iota(jnp.int32, (ref.shape[0], LANES), 0) == stage
        for n in range(nl):
            gains[which, n, 0:1, :] = jnp.sum(jnp.where(mine, ref[:, n * LANES:(n + 1) * LANES], 0.0), axis=0, keepdims=True)
    row_d = lax.broadcasted_iota(jnp.int32, (n_dec, LANES), 0)
    for table, out in ((cos_t, cosv), (sin_t, sinv)):
        out[0:seq_a, :] = table[0:seq_a, :]
        out[seq_a:row_b, :] = jnp.where(row_d == 0, table[pl.ds(len_a, 1), :], table[pl.ds(len_b, 1), :])
        out[row_b:n_rows, :] = table[pl.ds(pl.multiple_of(half * seq_b, seq_b), seq_b), :]

    for table, out in ((cos_t, 0), (sin_t, 1)):
        picked = jnp.where(row_d == 0, table[pl.ds(jnp.maximum(len_a - 1, 0), 1), :], table[pl.ds(jnp.maximum(len_b - 1, 0), 1), :])
        picked = jnp.where(row_d == 2, table[pl.ds(len_a, 1), :], picked)
        tsmall[out] = jnp.where(row_d == 3, table[pl.ds(len_b, 1), :], picked)

    def fill_mask(out, rows, offset, length):
        key = lax.broadcasted_iota(jnp.int32, (rows, LANES), 1)
        row = lax.broadcasted_iota(jnp.int32, (rows, LANES), 0) + offset
        return ((key <= row) & (key < length)).astype(f32)

    key_d = lax.broadcasted_iota(jnp.int32, (n_dec, LANES), 1)
    mask_a[0:seq_a, :] = fill_mask(mask_a, seq_a, 0, len_a)
    mask_a[seq_a:row_b, :] = (key_d < len_a).astype(f32)
    mask_b[0:n_dec, :] = (key_d < len_b).astype(f32)
    mask_b[n_dec:n_dec + seq_b, :] = fill_mask(mask_b, seq_b, half * seq_b, len_b)

    @pl.when(stage == 0)
    def _():
        for n in range(nl):
            acc = jnp.zeros((n_dec, LANES), f32)
            for b in range(n_prompts):
                take = ((row_d == 0) & (col == b)) | ((row_d == 1) & (half == 1) & (shared == b))
                acc = acc + jnp.where(take, new_ref[b:b + 1, n * LANES:(n + 1) * LANES].astype(f32), 0.0)
            xin[n, seq_a:row_b, :] = acc.astype(bf)
        for c in x0_copies():
            c.wait()

    def x_send(n):
        two = pl.ds(2 * n, 2)
        return pltpu.make_async_remote_copy(src_ref=xout.at[two], dst_ref=xin.at[two], send_sem=xs_sem.at[n], recv_sem=xr_sem.at[n],
                                            device_id={'model': lax.rem(stage + 1, stages), 'model2': col}, device_id_type=MESH)

    @pl.when(stage > 0)
    def _():
        for n in range(nx):
            x_send(n).wait_recv()

    def rms_into(src, which, dst):
        ss = jnp.zeros(src.shape[1:], f32)
        for n in range(nl):
            v = src[n].astype(f32)
            ss = ss + v * v
        inv = lax.rsqrt(jnp.sum(ss, axis=-1, keepdims=True) * (1.0 / d_model) + EPS)
        for n in range(nl):
            dst[n] = (src[n].astype(f32) * inv * gains[which, n, 0:1, :]).astype(bf)

    rms_into(xin, 0, hbuf)

    low = lax.broadcasted_iota(jnp.int32, (n_rows, LANES), 1) < head_dim

    def rope(y, cos, sin):
        lane = lax.broadcasted_iota(jnp.int32, y.shape, 1)
        first_half = lax.rem(lane, head_dim) < head_dim // 2
        swapped = jnp.where(first_half, pltpu.roll(y, LANES - head_dim // 2, 1), pltpu.roll(y, head_dim // 2, 1))
        return y * cos + swapped * sin

    wait_slot(0)
    wait_slot(1)
    h = cat(hbuf, 0, nl)
    k_all = dot_nn(h, weight(0))
    v_all = dot_nn(h, weight(1))
    for c in range(kv_heads):
        p = c // 2
        kk = rope(k_all[:, p * LANES:(p + 1) * LANES], cosv[...], sinv[...])
        vv = v_all[:, p * LANES:(p + 1) * LANES]
        if c % 2 == 0:
            packed = jnp.where(low, kk, pltpu.roll(vv, head_dim, 1))
        else:
            packed = jnp.where(low, pltpu.roll(kk, head_dim, 1), vv)
        kvp[c] = packed.astype(bf)

    pl.semaphore_wait(barrier, n_dev - 1)

    def pair_copy():
        return pltpu.make_async_remote_copy(src_ref=kvp.at[:, pl.ds(row_b, seq_b), :], dst_ref=kv_recv, send_sem=pair_sem.at[0], recv_sem=pair_sem.at[1],
                                            device_id={'model': stage, 'model2': col + 1 - 2 * half}, device_id_type=MESH)

    @pl.when(half == 0)
    def _():
        pair_copy().start()

    def queries(src, dst, cos, sin):
        def q_step(it, carry):
            for r in range(QU):
                wait_slot(2 + QU * it + r)
            h = cat(src, 0, nl)
            qs = [dot_nn(h, weight(2 + QU * it + r)) for r in range(QU)]
            for r in range(QU):
                for p in range(2):
                    dst[2 * (QU * it + r) + p] = rope(qs[r][:, p * LANES:(p + 1) * LANES], cos[...], sin[...]).astype(bf)
            return carry

        lax.fori_loop(0, nq // QU, q_step, 0)

    @pl.when(stage < last)
    def _():
        queries(hbuf, qbuf, cosv, sinv)
        for i in range(NSLOT, NSLOT + nq + 2):
            issue(i)

    @pl.when(half == 1)
    def _():
        pair_copy().wait_recv()

    low_s = lax.broadcasted_iota(jnp.int32, (seq_a, LANES), 1) < head_dim
    for c in range(kv_heads):
        own_b = kvp[c, row_b:row_b + seq_b, :]

        @pl.when(half == 0)
        def _():
            kvb[c, 2, 0:seq_b, :] = own_b

        @pl.when(half == 1)
        def _():
            kvb[c, 2, 0:seq_b, :] = kv_recv[c]

        kvb[c, 2, seq_b:2 * seq_b, :] = own_b
        for src, dst in ((kvp[c, 0:seq_a, :], kva), (kvb[c, 2, 0:seq_a, :], kvb)):
            f = src.astype(f32)
            r = pltpu.roll(f, head_dim, 1)
            dst[c, 0, 0:seq_a, :] = jnp.where(low_s, f, 0.0).astype(bf)
            dst[c, 0, seq_a:2 * seq_a, :] = jnp.where(low_s, 0.0, r).astype(bf)
            dst[c, 1, 0:seq_a, :] = jnp.where(low_s, r, 0.0).astype(bf)
            dst[c, 1, seq_a:2 * seq_a, :] = jnp.where(low_s, 0.0, f).astype(bf)

    def kv_copy(d, which, src_stage, prompt):
        return pltpu.make_async_remote_copy(src_ref=kvt.at[d // (per_head * width), which], dst_ref=kv_out.at[src_stage, prompt], send_sem=ks_sem.at[which, d],
                                            recv_sem=kr_sem.at[src_stage * n_prompts + prompt], device_id=device(d), device_id_type=MESH)

    def kv_local(which, prompt):
        return pltpu.make_async_copy(kvt.at[stage // per_head, which], kv_out.at[stage, prompt], ks_sem.at[which, me])

    own_rows = pl.ds(seq_a, n_dec)

    def dec_copy(d, src_stage, src_col):
        return pltpu.make_async_remote_copy(src_ref=kvp.at[d // (per_head * width), own_rows], dst_ref=dec_out.at[src_stage, src_col], send_sem=ks_sem.at[2, d],
                                            recv_sem=kd_sem.at[src_stage * width + src_col], device_id=device(d), device_id_type=MESH)

    def dec_local():
        return pltpu.make_async_copy(kvp.at[stage // per_head, own_rows], dec_out.at[stage, col], ks_sem.at[2, me])

    def kv_fill(which, src):
        for c in range(kv_heads):
            t = src(c).astype(f32).T
            for part in range(2):
                kvt[c, which, part] = t[part * head_dim:(part + 1) * head_dim].astype(bf)

    def others(step):
        def body(i, carry):
            step(lax.rem(me + i, n_dev))
            return carry

        lax.fori_loop(1, n_dev, body, 0)

    def kv_emit():
        others(lambda d: dec_copy(d, stage, col).start())
        dec_local().start()
        kv_fill(0, lambda c: kvp[c, 0:seq_a, :])
        others(lambda d: kv_copy(d, 0, stage, col).start())
        kv_local(0, col).start()

        @pl.when(half == 1)
        def _():
            kv_fill(1, lambda c: kvb[c, 2, 0:seq_a, :])
            others(lambda d: kv_copy(d, 1, stage, shared).start())
            kv_local(1, shared).start()

    scale = head_dim ** -0.5
    low_d = lax.broadcasted_iota(jnp.int32, (n_dec, LANES), 1) < head_dim

    def soft(s, mask):
        s = jnp.where(mask > 0, s * scale, NEG)
        m = jnp.max(s, axis=-1, keepdims=True)
        e = jnp.exp(s - m)
        return (e * (1.0 / jnp.sum(e, axis=-1, keepdims=True))).astype(bf)

    def soft_self(s, mask, s_self):
        s = jnp.where(mask > 0, s * scale, NEG)
        m = jnp.maximum(jnp.max(s, axis=-1, keepdims=True), s_self)
        e = jnp.exp(s - m)
        e_self = jnp.exp(s_self - m)
        inv = 1.0 / (jnp.sum(e, axis=-1, keepdims=True) + e_self)
        return (e * inv).astype(bf), (e_self * inv).astype(bf).astype(f32)

    pairs_per_kv = q_cols // (kv_heads * LANES)

    def kv_head(c, carry):
        kv_d = kvp[c, seq_a:row_b, :].astype(f32)
        kv_r = pltpu.roll(kv_d, head_dim, 1)
        k_self = jnp.where(low_d, kv_d, kv_r)
        v_self = jnp.where(low_d, kv_r, kv_d)
        for t in range(pairs_per_kv):
            hp = c * pairs_per_kv + t
            prod = qbuf[hp, seq_a:row_b, :].astype(f32) * k_self
            self_e = jnp.sum(jnp.where(low_d, prod, 0.0), axis=-1, keepdims=True) * scale
            self_o = jnp.sum(jnp.where(low_d, 0.0, prod), axis=-1, keepdims=True) * scale
            s_a = dot_nt(qbuf[hp, 0:row_b, :], kva[c, 0])
            s_b = dot_nt(qbuf[hp, seq_a:n_rows, :], kvb[c, 0])
            ma, mda = mask_a[0:seq_a, :], mask_a[seq_a:row_b, :]
            mdb, mb = mask_b[0:n_dec, :], mask_b[n_dec:n_dec + seq_b, :]
            pa = jnp.concatenate([soft(s_a[:seq_a, :seq_a], ma), soft(s_a[:seq_a, seq_a:], ma)], axis=1)
            pb = jnp.concatenate([soft(s_b[n_dec:, :seq_a], mb), soft(s_b[n_dec:, seq_a:], mb)], axis=1)
            dae, dae_s = soft_self(s_a[seq_a:, :seq_a], mda, self_e)
            dao, dao_s = soft_self(s_a[seq_a:, seq_a:], mda, self_o)
            dbe, dbe_s = soft_self(s_b[:n_dec, :seq_a], mdb, self_e)
            dbo, dbo_s = soft_self(s_b[:n_dec, seq_a:], mdb, self_o)
            o_a = dot_nn(jnp.concatenate([pa, jnp.concatenate([dae, dao], axis=1)], axis=0), kva[c, 1])
            o_b = dot_nn(jnp.concatenate([jnp.concatenate([dbe, dbo], axis=1), pb], axis=0), kvb[c, 1])
            o_da = o_a[seq_a:] + jnp.where(low_d, dae_s, dao_s) * v_self
            o_db = o_b[:n_dec] + jnp.where(low_d, dbe_s, dbo_s) * v_self
            hbuf[hp, 0:seq_a, :] = o_a[:seq_a].astype(bf)
            hbuf[hp, seq_a:row_b, :] = jnp.where(row_d == 0, o_da, o_db).astype(bf)
            hbuf[hp, row_b:n_rows, :] = o_b[n_dec:].astype(bf)
        return carry

    def project(src, res, dst):
        def out_step(it, carry):
            s0 = nq + 2 + QU * it
            for r in range(QU):
                wait_slot(s0 + r)
            o = cat(src, 0, nl)
            ys = [dot_nn(o, weight(s0 + r)) for r in range(QU)]
            for r in range(QU):
                for p in range(2):
                    n = 2 * (QU * it + r) + p
                    dst[n] = (res[n].astype(f32) + ys[r][:, p * LANES:(p + 1) * LANES]).astype(bf)
            return carry

        lax.fori_loop(0, nx // QU, out_step, 0)
        for i in range(NSLOT + nq + 2, NSLOT + n_attn):
            issue(i)

    n_loop = (NSLOT - n_attn) // 2 // GU * GU
    n_down = (len(order) - NSLOT - n_attn) // 2

    def gate_up(src, dst):
        def some(pairs):
            for j, sg in pairs:
                wait_slot(sg)
                wait_slot(sg + 1)
            h = cat(src, 0, nl)
            for j, sg in pairs:
                g = dot_nn(h, weight(sg))
                u = dot_nn(h, weight(sg + 1))
                a = (g * (1.0 / (1.0 + jnp.exp(-g))) * u).astype(bf)
                dst[2 * j] = a[:, :LANES]
                dst[2 * j + 1] = a[:, LANES:]

        def gu_step(it, carry):
            some([(GU * it + r, n_attn + 2 * (GU * it + r)) for r in range(GU)])

            @pl.when(it < n_down // GU)
            def _():
                for r in range(2 * GU):
                    ring_start(w_dt, NSLOT + n_attn - n_up + 2 * GU * it + r, n_attn + 2 * GU * it + r)
            return carry

        lax.fori_loop(0, n_loop // GU, gu_step, 0)
        some([(j, (n_attn + 2 * j) % NSLOT) for j in range(n_loop, nff)])

    d_slots = [(n_up + k) % NSLOT for k in range(nff)]

    def down(src, res, dst, send):
        for s in d_slots:
            wait_slot(s)

        def down_step(n, carry):
            ys = []
            for t in range(2):
                rows = pl.ds(pl.multiple_of((2 * n + t) * BLK, BLK), BLK)
                acc = None
                for k in range(nff):
                    w = jnp.concatenate([ring[2 * d_slots[k], rows, :], ring[2 * d_slots[k] + 1, rows, :]], axis=1)
                    y = dot_nt(cat(src, 2 * k, 2), w)
                    acc = y if acc is None else acc + y
                ys.append(acc)
            for t in range(2):
                for p in range(2):
                    i = 2 * (2 * n + t) + p
                    dst[i] = (res[i].astype(f32) + ys[t][:, p * LANES:(p + 1) * LANES]).astype(bf)
            if send:
                x_send(2 * n).start()
                x_send(2 * n + 1).start()
            return carry

        lax.fori_loop(0, nx // 2, down_step, 0)

    @pl.when(stage < last)
    def _():
        lax.fori_loop(0, kv_heads, kv_head, 0)
        project(hbuf, xin, x1buf)
        rms_into(x1buf, 1, hbuf)
        gate_up(hbuf, abuf)
        down(abuf, x1buf, xout, True)
        kv_emit()

    def res_copy(d, src_col):
        return pltpu.make_async_remote_copy(src_ref=res_vm, dst_ref=res_out.at[src_col], send_sem=rs_sem.at[d], recv_sem=rr_sem.at[src_col],
                                            device_id=device(d), device_id_type=MESH)

    def res_local():
        return pltpu.make_async_copy(res_vm, res_out.at[col], rs_sem.at[me])

    groups = n_dec // 4

    @pl.when(stage == last)
    def _():
        xs, hs, qs, x1s, ys = (small.at[i] for i in range(5))
        who = lax.broadcasted_iota(jnp.int32, (n_dec, n_rows), 0)
        at = lax.broadcasted_iota(jnp.int32, (n_dec, n_rows), 1)
        off_b = len_b - 1 - half * seq_b
        hit = ((who == 0) & (at == len_a - 1)) | ((who == 1) & (at >= row_b) & (at == row_b + off_b)) | ((who == 2) & (at == seq_a)) | ((who == 3) & (half == 1) & (at == seq_a + 1))
        sel = jnp.where(hit, 1.0, 0.0).astype(bf)
        for n in range(nl // 2):
            for src, dst in ((xin, xs), (hbuf, hs)):
                y = dot_nn(sel, cat(src, 2 * n, 2)).astype(bf)
                dst[2 * n] = y[:, :LANES]
                dst[2 * n + 1] = y[:, LANES:]
        queries(hs, qs, tsmall.at[0], tsmall.at[1])
        for i in range(NSLOT, NSLOT + nq + 2):
            issue(i)
        kv_emit()

        stack = pairs_per_kv * n_dec
        key = lax.broadcasted_iota(jnp.int32, (stack, LANES), 1)
        row = lax.rem(lax.broadcasted_iota(jnp.int32, (stack, LANES), 0), n_dec)
        low_k = key < head_dim
        mk_a, mk_b = (key < len_a).astype(f32), (key < len_b).astype(f32)
        decode = (row[:, 0:1] == 2) | (row[:, 0:1] == 3)
        from_a = lax.rem(row, 2) == 0
        for c in range(kv_heads):
            kd = kvp[c, seq_a:row_b, :].astype(f32)
            kr = pltpu.roll(kd, head_dim, 1)
            k_two, v_two = jnp.where(low_d, kd, kr), jnp.where(low_d, kr, kd)
            k_self = jnp.where(from_a, k_two[0:1], k_two[1:2])
            v_self = jnp.where(from_a, v_two[0:1], v_two[1:2])
            q4 = jnp.concatenate([qs[c * pairs_per_kv + t] for t in range(pairs_per_kv)], axis=0)
            prod = q4.astype(f32) * k_self
            self_e = jnp.where(decode, jnp.sum(jnp.where(low_k, prod, 0.0), axis=-1, keepdims=True) * scale, NEG)
            self_o = jnp.where(decode, jnp.sum(jnp.where(low_k, 0.0, prod), axis=-1, keepdims=True) * scale, NEG)
            outs = []
            for kv, mk in ((kva, mk_a), (kvb, mk_b)):
                sc = dot_nt(q4, kv[c, 0])
                pe, pe_s = soft_self(sc[:, :seq_a], mk, self_e)
                po, po_s = soft_self(sc[:, seq_a:], mk, self_o)
                outs.append(dot_nn(jnp.concatenate([pe, po], axis=1), kv[c, 1]) + jnp.where(low_k, pe_s, po_s) * v_self)
            o = jnp.where(from_a, outs[0], outs[1]).astype(bf)
            for t in range(pairs_per_kv):
                hs[c * pairs_per_kv + t] = o[t * n_dec:(t + 1) * n_dec]

        project(hs, xs, x1s)
        rms_into(x1s, 1, hs)
        gate_up(hs, asmall)
        down(asmall, x1s, ys, False)
        keep = (row_d == 0) | (row_d == 2) | ((row_d == 1) & (off_b >= 0) & (off_b < seq_b)) | ((row_d == 3) & (half == 1))
        for n in range(2 * nx // groups):
            j, p = n // 2, n % 2
            acc = jnp.zeros((n_dec, LANES), f32)
            for i in range(groups):
                y = jnp.where(keep, ys[2 * (groups * j + i) + p].astype(f32), 0.0)
                y = pltpu.roll(y, 4 * i, 0) if i else y
                acc = jnp.where(row_d // 4 == i, y, acc)
            res_vm[:, n * LANES:(n + 1) * LANES] = acc.astype(bf)
        others(lambda d: res_copy(d, col).start())
        res_local().start()
        others(lambda d: res_copy(d, col).wait_send())
        res_local().wait()

    @pl.when(stage < last)
    def _():
        for n in range(nx):
            x_send(n).wait_send()

    @pl.when(half == 0)
    def _():
        pair_copy().wait_send()

    others(lambda d: dec_copy(d, stage, col).wait_send())
    dec_local().wait()
    others(lambda d: kv_copy(d, 0, stage, col).wait_send())
    kv_local(0, col).wait()

    @pl.when(half == 1)
    def _():
        others(lambda d: kv_copy(d, 1, stage, shared).wait_send())
        kv_local(1, shared).wait()

    others(lambda d: dec_copy(0, d // width, lax.rem(d, width)).wait_recv())
    for b in range(n_prompts):
        owner = b if b < width else 2 * (b - width) + 1

        def kv_in(s, carry, b=b, owner=owner):
            @pl.when((s != stage) | (col != owner))
            def _():
                kv_copy(0, 0, s, b).wait_recv()
            return carry

        lax.fori_loop(0, stages, kv_in, 0)

    def res_in(y, carry):
        @pl.when((stage != last) | (y != col))
        def _():
            res_copy(0, y).wait_recv()
        return carry

    lax.fori_loop(0, width, res_in, 0)


def solution(mesh):
    stages = mesh.shape['model']
    width = mesh.shape['model2']
    stage_spec = P('model', None, None)
    in_specs = (P('replica', None, None, None), P('replica', None), P('replica', None),
                stage_spec, stage_spec, stage_spec, stage_spec, P(None, None), P(None, None),
                P(None, None, TP_AXES, None), P(None, None, TP_AXES, None), P(None, None, TP_AXES, None),
                P(None, TP_AXES, None, None), P(None, None, TP_AXES), P(None, None, TP_AXES), P(None, TP_AXES, None))
    cache_spec = P(None, 'replica', None, TP_AXES, None)
    out_specs = (P('replica', None), P('replica', None), cache_spec, cache_spec)

    def shard_body(x_prompt, lengths, x_new, st_qkv, st_out, st_gateup, st_down_t, gain_attn, gain_mlp, tp_query, tp_key, tp_value, tp_out, tp_gate, tp_up, tp_down):
        n_prompts, _, seq_len, d_model = x_prompt.shape
        head_dim = tp_query.shape[-1]
        q_cols = st_out.shape[1]
        kv_heads = (st_qkv.shape[2] - q_cols) // (2 * head_dim)
        ff = st_down_t.shape[2]
        n_dec = 16
        seq_a, seq_b = seq_len, seq_len // 2
        assert n_prompts == width + width // 2 and st_qkv.shape[0] == 1 and tp_key.shape[2] == 1
        n_rows = seq_a + n_dec + seq_b
        groups = n_dec // 4
        bf, f32 = jnp.bfloat16, jnp.float32
        cos_t, sin_t = rope_table(seq_len + 8, head_dim)
        dims = (stages, width, kv_heads, head_dim, seq_a, seq_b, n_dec, q_cols, ff, n_prompts)
        nx, nl = d_model // BLK, d_model // LANES
        n_dev = stages * width
        vmem, hbm = pl.BlockSpec(memory_space=pltpu.VMEM), pl.BlockSpec(memory_space=pl.ANY)
        smem = pl.BlockSpec(memory_space=pltpu.SMEM)
        dma = pltpu.SemaphoreType.DMA
        kv_all, dec_all, res = pl.pallas_call(
            functools.partial(stage_kernel, dims),
            out_shape=(jax.ShapeDtypeStruct((stages, n_prompts, 2, head_dim, seq_len), bf), jax.ShapeDtypeStruct((stages, width, n_dec, LANES), bf), jax.ShapeDtypeStruct((width, n_dec, d_model // groups), bf)),
            in_specs=[smem] + [vmem] * 5 + [hbm] * 5,
            out_specs=(hbm, hbm, hbm),
            scratch_shapes=[
                pltpu.VMEM((2 * NSLOT, d_model, LANES), bf),
                pltpu.VMEM((nl, n_rows, LANES), bf),
                pltpu.VMEM((nl, n_rows, LANES), bf),
                pltpu.VMEM((nl, n_rows, LANES), bf),
                pltpu.VMEM((q_cols // LANES, n_rows, LANES), bf),
                pltpu.VMEM((nl, n_rows, LANES), bf),
                pltpu.VMEM((ff // LANES, n_rows, LANES), bf),
                pltpu.VMEM((kv_heads, n_rows, LANES), bf),
                pltpu.VMEM((kv_heads, 2, 2 * seq_a, LANES), bf),
                pltpu.VMEM((kv_heads, 3, 2 * seq_a, LANES), bf),
                pltpu.VMEM((kv_heads, seq_b, LANES), bf),
                pltpu.VMEM((kv_heads, 2, 2, head_dim, seq_len), bf),
                pltpu.VMEM((n_rows, LANES), f32),
                pltpu.VMEM((n_rows, LANES), f32),
                pltpu.VMEM((2, nl, 8, LANES), f32),
                pltpu.VMEM((seq_a + n_dec, LANES), f32),
                pltpu.VMEM((n_dec + seq_b, LANES), f32),
                pltpu.VMEM((n_dec, d_model // groups), bf),
                pltpu.VMEM((5, nl, n_dec, LANES), bf),
                pltpu.VMEM((ff // LANES, n_dec, LANES), bf),
                pltpu.VMEM((2, n_dec, LANES), f32),
                dma((2 * NSLOT,)), dma((2 * nl,)), dma((nx,)), dma((nx,)), dma((3, n_dev)), dma((stages * n_prompts,)), dma((n_dev,)), dma((n_dev,)), dma((width,)), dma((2,)),
            ],
            compiler_params=pltpu.CompilerParams(collective_id=0, has_side_effects=True, vmem_limit_bytes=67043328),
        )(lengths, cos_t, sin_t, gain_attn, gain_mlp, x_new, x_prompt, st_qkv, st_out, st_gateup, st_down_t)

        picked = res.reshape(width, groups, 4, nx // groups, BLK).transpose(0, 2, 3, 1, 4).reshape(width, 4, d_model)
        last_hidden = jnp.concatenate([picked[:, 0], picked[0::2, 1] + picked[1::2, 1]], axis=0)
        dec_out = jnp.concatenate([picked[:, 2], picked[1::2, 3]], axis=0)

        dec_kv = jnp.concatenate([dec_all[:, :, 0], dec_all[:, 1::2, 1]], axis=1)

        def cache(part):
            own = dec_kv[:, :, part * head_dim:(part + 1) * head_dim]
            return jnp.concatenate([kv_all[:, :, part], own[..., None]], axis=3).transpose(0, 1, 3, 2)[:, :, :, None, :]

        return dec_out, last_hidden, cache(0), cache(1)

    return jax.shard_map(shard_body, mesh=mesh, in_specs=in_specs, out_specs=out_specs, check_vma=False)
```

```python
import functools

import jax
import jax.numpy as jnp
import numpy as np
from jax import lax
from jax.experimental import pallas as pl
from jax.experimental.pallas import tpu as pltpu
from jax.sharding import PartitionSpec as P

EPS = 1e-5
THETA = 10000.0
TP_AXES = ('model', 'model2')
MESH = pl.DeviceIdType.MESH
BLK = 256
LANES = 128
NSLOT = 32
NEG = -1e30
QU = 4
GU = 4


def rope_table(count, head_dim):
    half_dim = head_dim // 2
    inv_freq = np.power(np.float32(THETA), np.arange(half_dim, dtype=np.float32) * np.float32(-2.0 / head_dim))
    angles = (np.arange(count, dtype=np.float32)[:, None] * inv_freq.astype(np.float32)).astype(np.float64)
    cos, sin = np.cos(angles).astype(np.float32), np.sin(angles).astype(np.float32)
    return jnp.asarray(np.tile(cos, (1, 2 * LANES // head_dim))), jnp.asarray(np.tile(np.concatenate([-sin, sin], axis=1), (1, LANES // head_dim)))


def dot_nn(a, b):
    return lax.dot_general(a, b, (((1,), (0,)), ((), ())), preferred_element_type=jnp.float32)


def dot_nt(a, b):
    return lax.dot_general(a, b, (((1,), (1,)), ((), ())), preferred_element_type=jnp.float32)


def cat(ref, first, count):
    return jnp.concatenate([ref[first + t] for t in range(count)], axis=1)


def stage_kernel(dims, lens_ref, cos_t, sin_t, ga_ref, gm_ref, new_ref, x_hbm, w_qkv, w_out, w_gu, w_dt, kv_out, dec_out, res_out,
                 ring, dbuf, xin_a, xin_b, xout_a, xout_b, h_a, h_b, qbuf, x1buf, abuf, kvp_a, kvp_b, kva, kvb, kv_recv, kvt, kvd, tab_a, tab_b, gains, mask_a, mask_b, res_vm, small, asmall, tsmall,
                 ring_sem, d_sem, x0_sem, xs_sem, xr_sem, ks_sem, kr_sem, kd_sem, rs_sem, rr_sem, pair_sem):
    stages, width, kv_heads, head_dim, seq_a, seq_b, n_dec, q_cols, ff, n_prompts = dims
    rows_a, rows_b = seq_a + n_dec, seq_b + n_dec
    d_model = w_out.shape[2]
    nx = d_model // BLK
    nl = d_model // LANES
    nq = q_cols // BLK
    nff = ff // BLK
    n_dev = stages * width
    per_head = stages // kv_heads
    last = stages - 1
    bf, f32 = jnp.bfloat16, jnp.float32
    stage = lax.axis_index('model')
    col = lax.axis_index('model2')
    me = stage * width + col
    half = lax.rem(col, 2)
    shared = width + col // 2
    len_a = lens_ref[col, 0]
    len_b = lens_ref[shared, 0]

    def ring_copy(ref, c, slot, t):
        start = pl.multiple_of(c * BLK + t * LANES, LANES)
        return pltpu.make_async_copy(ref.at[0, :, pl.ds(start, LANES)], ring.at[2 * slot + t], ring_sem.at[2 * slot + t])

    def ring_start(ref, c, slot):
        ring_copy(ref, c, slot, 0).start()
        ring_copy(ref, c, slot, 1).start()

    def wait_slot(slot):
        ring_copy(w_out, 0, slot, 0).wait()
        ring_copy(w_out, 0, slot, 1).wait()

    def weight(slot):
        return cat(ring, 2 * slot, 2)

    order = [(w_qkv, nq), (w_qkv, nq + 1)] + [(w_qkv, c) for c in range(nq)] + [(w_out, c) for c in range(nx)]
    n_attn = len(order)
    for j in range(nff):
        order += [(w_gu, j), (w_gu, nff + j)]
    n_up = len(order)

    def issue(base, i):
        ref, c = order[i % len(order)]
        ring_start(ref, c, (base + i) % NSLOT)

    def x0_copies():
        out = []
        for n in range(nl):
            cs = pl.ds(n * LANES, LANES)
            out.append(pltpu.make_async_copy(x_hbm.at[col, 0, :, cs], xin_a.at[n, pl.ds(0, seq_a), :], x0_sem.at[2 * n]))
            out.append(pltpu.make_async_copy(x_hbm.at[shared, 0, pl.ds(pl.multiple_of(half * seq_b, seq_b), seq_b), cs], xin_b.at[n, pl.ds(0, seq_b), :], x0_sem.at[2 * n + 1]))
        return out

    @pl.when(stage == 0)
    def _():
        for c in x0_copies():
            c.start()

    for i in range(NSLOT):
        issue(0, i)

    def d_copy(k):
        return pltpu.make_async_copy(w_dt.at[0, :, pl.ds(k * LANES, LANES)], dbuf.at[k], d_sem.at[k])

    @pl.when(stage > 0)
    def _():
        for k in range(2 * nff):
            d_copy(k).start()

    barrier = pltpu.get_barrier_semaphore()

    def device(d):
        return {'model': d // width, 'model2': lax.rem(d, width)}

    def greet(i, carry):
        pl.semaphore_signal(barrier, inc=1, device_id=device(lax.rem(me + i, n_dev)), device_id_type=MESH)
        return carry

    lax.fori_loop(1, n_dev, greet, 0)

    for which, ref in ((0, ga_ref), (1, gm_ref)):
        mine = lax.broadcasted_iota(jnp.int32, (ref.shape[0], LANES), 0) == stage
        for n in range(nl):
            gains[which, n, 0:1, :] = jnp.sum(jnp.where(mine, ref[:, n * LANES:(n + 1) * LANES], 0.0), axis=0, keepdims=True)
    row_d = lax.broadcasted_iota(jnp.int32, (n_dec, LANES), 0)
    for k, table in enumerate((cos_t, sin_t)):
        tab_a[k, 0:seq_a, :] = table[0:seq_a, :]
        tab_a[k, seq_a:rows_a, :] = jnp.broadcast_to(table[pl.ds(len_a, 1), :], (n_dec, LANES))
        tab_b[k, 0:seq_b, :] = table[pl.ds(pl.multiple_of(half * seq_b, seq_b), seq_b), :]
        tab_b[k, seq_b:rows_b, :] = jnp.broadcast_to(table[pl.ds(len_b, 1), :], (n_dec, LANES))
    for table, out in ((cos_t, 0), (sin_t, 1)):
        picked = jnp.where(row_d == 0, table[pl.ds(jnp.maximum(len_a - 1, 0), 1), :], table[pl.ds(jnp.maximum(len_b - 1, 0), 1), :])
        picked = jnp.where(row_d == 2, table[pl.ds(len_a, 1), :], picked)
        tsmall[out] = jnp.where(row_d == 3, table[pl.ds(len_b, 1), :], picked)

    def fill_mask(out, rows, offset, length):
        key = lax.broadcasted_iota(jnp.int32, (rows, LANES), 1)
        row = lax.broadcasted_iota(jnp.int32, (rows, LANES), 0) + offset
        out[0:rows, :] = ((key <= row) & (key < length)).astype(f32)
        key = lax.broadcasted_iota(jnp.int32, (n_dec, LANES), 1)
        out[rows:rows + n_dec, :] = (key < length).astype(f32)

    fill_mask(mask_a, seq_a, 0, len_a)
    fill_mask(mask_b, seq_b, half * seq_b, len_b)

    @pl.when(stage == 0)
    def _():
        for n in range(nl):
            for dst, lo, want in ((xin_a, seq_a, col), (xin_b, seq_b, jnp.where(half == 1, shared, -1))):
                acc = jnp.zeros((n_dec, LANES), f32)
                for b in range(n_prompts):
                    acc = acc + jnp.where((row_d == 0) & (want == b), new_ref[b:b + 1, n * LANES:(n + 1) * LANES].astype(f32), 0.0)
                dst[n, lo:lo + n_dec, :] = acc.astype(bf)
        for c in x0_copies():
            c.wait()

    def x_send(k, n):
        two = pl.ds(2 * n, 2)
        src, dst = ((xout_a, xin_a), (xout_b, xin_b))[k]
        return pltpu.make_async_remote_copy(src_ref=src.at[two], dst_ref=dst.at[two], send_sem=xs_sem.at[k, n], recv_sem=xr_sem.at[k, n],
                                            device_id={'model': lax.rem(stage + 1, stages), 'model2': col}, device_id_type=MESH)

    def x_arrive(k):
        @pl.when(stage > 0)
        def _():
            for n in range(nx):
                x_send(k, n).wait_recv()

    def rms_into(src, which, dst):
        ss = jnp.zeros(src.shape[1:], f32)
        for n in range(nl):
            v = src[n].astype(f32)
            ss = ss + v * v
        inv = lax.rsqrt(jnp.sum(ss, axis=-1, keepdims=True) * (1.0 / d_model) + EPS)
        for n in range(nl):
            dst[n] = (src[n].astype(f32) * inv * gains[which, n, 0:1, :]).astype(bf)

    def rope(y, cos, sin):
        lane = lax.broadcasted_iota(jnp.int32, y.shape, 1)
        first_half = lax.rem(lane, head_dim) < head_dim // 2
        swapped = jnp.where(first_half, pltpu.roll(y, LANES - head_dim // 2, 1), pltpu.roll(y, head_dim // 2, 1))
        return y * cos + swapped * sin

    def keys_values(src, tab, dst, slot):
        h = cat(src, 0, nl)
        k_all = dot_nn(h, weight(slot))
        v_all = dot_nn(h, weight(lax.rem(slot + 1, NSLOT)))
        low = lax.broadcasted_iota(jnp.int32, (src.shape[1], LANES), 1) < head_dim
        for c in range(kv_heads):
            p = c // 2
            kk = rope(k_all[:, p * LANES:(p + 1) * LANES], tab[0], tab[1])
            vv = v_all[:, p * LANES:(p + 1) * LANES]
            if c % 2 == 0:
                packed = jnp.where(low, kk, pltpu.roll(vv, head_dim, 1))
            else:
                packed = jnp.where(low, pltpu.roll(kk, head_dim, 1), vv)
            dst[c] = packed.astype(bf)

    def pair_copy():
        return pltpu.make_async_remote_copy(src_ref=kvp_b.at[:, pl.ds(0, seq_b), :], dst_ref=kv_recv, send_sem=pair_sem.at[0], recv_sem=pair_sem.at[1],
                                            device_id={'model': stage, 'model2': col + 1 - 2 * half}, device_id_type=MESH)

    def queries(base, src, dst, cos, sin):
        def q_step(it, carry):
            sl = [lax.rem(base + 2 + QU * it + r, NSLOT) for r in range(QU)]
            for t in sl:
                wait_slot(t)
            h = cat(src, 0, nl)
            qs = [dot_nn(h, weight(t)) for t in sl]
            for r in range(QU):
                for p in range(2):
                    dst[2 * (QU * it + r) + p] = rope(qs[r][:, p * LANES:(p + 1) * LANES], cos[...], sin[...]).astype(bf)
            return carry

        lax.fori_loop(0, nq // QU, q_step, 0)
        for i in range(NSLOT, NSLOT + nq + 2):
            issue(base, i)

    low_s = lax.broadcasted_iota(jnp.int32, (seq_a, LANES), 1) < head_dim

    def widen(src, dst, c):
        f = src.astype(f32)
        r = pltpu.roll(f, head_dim, 1)
        dst[c, 0, 0:seq_a, :] = jnp.where(low_s, f, 0.0).astype(bf)
        dst[c, 0, seq_a:2 * seq_a, :] = jnp.where(low_s, 0.0, r).astype(bf)
        dst[c, 1, 0:seq_a, :] = jnp.where(low_s, r, 0.0).astype(bf)
        dst[c, 1, seq_a:2 * seq_a, :] = jnp.where(low_s, 0.0, f).astype(bf)

    def widen_b():
        for c in range(kv_heads):
            own_b = kvp_b[c, 0:seq_b, :]

            @pl.when(half == 0)
            def _():
                kvb[c, 2, 0:seq_b, :] = own_b

            @pl.when(half == 1)
            def _():
                kvb[c, 2, 0:seq_b, :] = kv_recv[c]

            kvb[c, 2, seq_b:2 * seq_b, :] = own_b
            widen(kvb[c, 2, 0:seq_a, :], kvb, c)

    def kv_copy(d, which, src_stage, prompt):
        return pltpu.make_async_remote_copy(src_ref=kvt.at[d // (per_head * width), which], dst_ref=kv_out.at[src_stage, prompt], send_sem=ks_sem.at[which, d],
                                            recv_sem=kr_sem.at[src_stage * n_prompts + prompt], device_id=device(d), device_id_type=MESH)

    def kv_local(which, prompt):
        return pltpu.make_async_copy(kvt.at[stage // per_head, which], kv_out.at[stage, prompt], ks_sem.at[which, me])

    def dec_copy(d, src_stage, src_col):
        return pltpu.make_async_remote_copy(src_ref=kvd.at[d // (per_head * width)], dst_ref=dec_out.at[src_stage, src_col], send_sem=ks_sem.at[2, d],
                                            recv_sem=kd_sem.at[src_stage * width + src_col], device_id=device(d), device_id_type=MESH)

    def dec_local():
        return pltpu.make_async_copy(kvd.at[stage // per_head], dec_out.at[stage, col], ks_sem.at[2, me])

    def kv_fill(which, src):
        for c in range(kv_heads):
            t = src(c).astype(f32).T
            for part in range(2):
                kvt[c, which, part] = t[part * head_dim:(part + 1) * head_dim].astype(bf)

    def others(step):
        def body(i, carry):
            step(lax.rem(me + i, n_dev))
            return carry

        lax.fori_loop(1, n_dev, body, 0)

    def emit_a():
        kv_fill(0, lambda c: kvp_a[c, 0:seq_a, :])
        others(lambda d: kv_copy(d, 0, stage, col).start())
        kv_local(0, col).start()

    def emit_b():
        for c in range(kv_heads):
            other = pltpu.roll(kvp_b[c, seq_b:rows_b, :].astype(f32), 1, 0)
            kvd[c] = jnp.where(row_d == 0, kvp_a[c, seq_a:rows_a, :].astype(f32), other).astype(bf)
        others(lambda d: dec_copy(d, stage, col).start())
        dec_local().start()

        @pl.when(half == 1)
        def _():
            kv_fill(1, lambda c: kvb[c, 2, 0:seq_a, :])
            others(lambda d: kv_copy(d, 1, stage, shared).start())
            kv_local(1, shared).start()

    scale = head_dim ** -0.5
    low_d = lax.broadcasted_iota(jnp.int32, (n_dec, LANES), 1) < head_dim

    def soft(s, mask):
        s = jnp.where(mask > 0, s * scale, NEG)
        m = jnp.max(s, axis=-1, keepdims=True)
        e = jnp.exp(s - m)
        return (e * (1.0 / jnp.sum(e, axis=-1, keepdims=True))).astype(bf)

    def soft_self(s, mask, s_self):
        s = jnp.where(mask > 0, s * scale, NEG)
        m = jnp.maximum(jnp.max(s, axis=-1, keepdims=True), s_self)
        e = jnp.exp(s - m)
        e_self = jnp.exp(s_self - m)
        inv = 1.0 / (jnp.sum(e, axis=-1, keepdims=True) + e_self)
        return (e * inv).astype(bf), (e_self * inv).astype(bf).astype(f32)

    pairs_per_kv = q_cols // (kv_heads * LANES)

    def attend(kvp, kv, mask, n_main, dst):
        n_all = n_main + n_dec

        def kv_head(c, carry):
            kv_d = kvp[c, n_main:n_all, :].astype(f32)
            kv_r = pltpu.roll(kv_d, head_dim, 1)
            k_self = jnp.where(low_d, kv_d, kv_r)
            v_self = jnp.where(low_d, kv_r, kv_d)
            for t in range(pairs_per_kv):
                hp = c * pairs_per_kv + t
                prod = qbuf[hp, n_main:n_all, :].astype(f32) * k_self
                self_e = jnp.sum(jnp.where(low_d, prod, 0.0), axis=-1, keepdims=True) * scale
                self_o = jnp.sum(jnp.where(low_d, 0.0, prod), axis=-1, keepdims=True) * scale
                sc = dot_nt(qbuf[hp, 0:n_all, :], kv[c, 0])
                mm, md = mask[0:n_main, :], mask[n_main:n_all, :]
                pm = jnp.concatenate([soft(sc[:n_main, :seq_a], mm), soft(sc[:n_main, seq_a:], mm)], axis=1)
                de, de_s = soft_self(sc[n_main:, :seq_a], md, self_e)
                do, do_s = soft_self(sc[n_main:, seq_a:], md, self_o)
                o = dot_nn(jnp.concatenate([pm, jnp.concatenate([de, do], axis=1)], axis=0), kv[c, 1])
                dst[hp, 0:n_main, :] = o[:n_main].astype(bf)
                dst[hp, n_main:n_all, :] = (o[n_main:] + jnp.where(low_d, de_s, do_s) * v_self).astype(bf)
            return carry

        lax.fori_loop(0, kv_heads, kv_head, 0)

    def project(base, src, res, dst):
        def out_step(it, carry):
            sl = [lax.rem(base + nq + 2 + QU * it + r, NSLOT) for r in range(QU)]
            for t in sl:
                wait_slot(t)
            o = cat(src, 0, nl)
            ys = [dot_nn(o, weight(t)) for t in sl]
            for r in range(QU):
                for p in range(2):
                    n = 2 * (QU * it + r) + p
                    dst[n] = (res[n].astype(f32) + ys[r][:, p * LANES:(p + 1) * LANES]).astype(bf)
            return carry

        lax.fori_loop(0, nx // QU, out_step, 0)
        for i in range(NSLOT + nq + 2, NSLOT + n_attn):
            issue(base, i)

    n_loop = nff // GU * GU

    def gate_up(base, src, dst, again):
        def some(pairs):
            for j, sg in pairs:
                wait_slot(sg)
                wait_slot(lax.rem(sg + 1, NSLOT))
            h = cat(src, 0, nl)
            for j, sg in pairs:
                g = dot_nn(h, weight(sg))
                u = dot_nn(h, weight(lax.rem(sg + 1, NSLOT)))
                a = (g * (1.0 / (1.0 + jnp.exp(-g))) * u).astype(bf)
                dst[2 * j] = a[:, :LANES]
                dst[2 * j + 1] = a[:, LANES:]

        def gu_step(it, carry):
            some([(GU * it + r, lax.rem(base + n_attn + 2 * (GU * it + r), NSLOT)) for r in range(GU)])

            for k in range(n_loop // GU):
                todo = [i for i in range(NSLOT + n_attn + 2 * GU * k, NSLOT + n_attn + 2 * GU * (k + 1)) if again or i < len(order)]
                if todo:
                    @pl.when(it == k)
                    def _(todo=todo):
                        for i in todo:
                            issue(base, i)
            return carry

        lax.fori_loop(0, n_loop // GU, gu_step, 0)
        for lo in range(n_loop, nff, GU):
            some([(j, jnp.int32((base + n_attn + 2 * j) % NSLOT)) for j in range(lo, min(lo + GU, nff))])
        if again:
            for i in range(NSLOT + n_attn + 2 * n_loop, NSLOT + n_up):
                issue(base, i)

    def down(src, res, dst, k_send, flipped):
        def down_step(n, carry):
            ys = []
            for t in range(2):
                lo = pl.multiple_of((2 * n + t) * BLK, BLK)
                acc = None
                for k in range(nff):
                    if flipped:
                        r0, r1 = pl.ds(lo, LANES), pl.ds(pl.multiple_of(lo + LANES, LANES), LANES)
                        w = jnp.concatenate([jnp.concatenate([dbuf[2 * k + i, r0, :], dbuf[2 * k + i, r1, :]], axis=1) for i in range(2)], axis=0)
                        y = dot_nn(cat(src, 2 * k, 2), w)
                    else:
                        rows = pl.ds(lo, BLK)
                        y = dot_nt(cat(src, 2 * k, 2), jnp.concatenate([dbuf[2 * k, rows, :], dbuf[2 * k + 1, rows, :]], axis=1))
                    acc = y if acc is None else acc + y
                ys.append(acc)
            for t in range(2):
                for p in range(2):
                    i = 2 * (2 * n + t) + p
                    dst[i] = (res[i].astype(f32) + ys[t][:, p * LANES:(p + 1) * LANES]).astype(bf)
            if k_send is not None:
                x_send(k_send, 2 * n).start()
                x_send(k_send, 2 * n + 1).start()
            return carry

        lax.fori_loop(0, nx // 2, down_step, 0)

    @pl.when(stage > 0)
    def _():
        for k in range(2 * nff):
            d_copy(k).wait()

        def flip(k, carry):
            for i in range(nl):
                tile = slice(i * LANES, (i + 1) * LANES)
                dbuf[k, tile, :] = dbuf[k, tile, :].astype(f32).T.astype(bf)
            return carry

        lax.fori_loop(0, 2 * nff, flip, 0)

    wait_slot(0)
    wait_slot(1)
    x_arrive(0)
    rms_into(xin_a, 0, h_a)
    keys_values(h_a, tab_a, kvp_a, 0)
    for c in range(kv_heads):
        widen(kvp_a[c, 0:seq_a, :], kva, c)
    part_a, part_b = pl.ds(0, rows_a), pl.ds(0, rows_b)

    @pl.when(stage < last)
    def _():
        q_a = qbuf.at[:, part_a, :]
        queries(0, h_a, q_a, tab_a.at[0], tab_a.at[1])
        attend(kvp_a, kva, mask_a, seq_a, h_a)
        project(0, h_a, xin_a, x1buf.at[:, part_a, :])

        @pl.when(stage == 0)
        def _():
            for k in range(2 * nff):
                d_copy(k).start()

    pl.semaphore_wait(barrier, n_dev - 1)

    @pl.when(stage < last)
    def _():
        rms_into(x1buf.at[:, part_a, :], 1, h_a)
        gate_up(0, h_a, abuf.at[:, part_a, :], True)
        @pl.when(stage == 0)
        def _():
            for k in range(2 * nff):
                d_copy(k).wait()
            down(abuf.at[:, part_a, :], x1buf.at[:, part_a, :], xout_a, 0, False)

        @pl.when(stage > 0)
        def _():
            down(abuf.at[:, part_a, :], x1buf.at[:, part_a, :], xout_a, 0, True)

    second = len(order)
    kv_slot = jnp.where(stage < last, second % NSLOT, 0)

    @pl.when(stage < last)
    def _():
        wait_slot(second % NSLOT)
        wait_slot((second + 1) % NSLOT)

    x_arrive(1)
    rms_into(xin_b, 0, h_b)
    keys_values(h_b, tab_b, kvp_b, kv_slot)

    @pl.when(half == 0)
    def _():
        pair_copy().start()

    @pl.when(stage < last)
    def _():
        queries(second, h_b, qbuf.at[:, part_b, :], tab_b.at[0], tab_b.at[1])

    @pl.when(stage == last)
    def _():
        emit_a()

    @pl.when(half == 1)
    def _():
        pair_copy().wait_recv()

    widen_b()

    @pl.when(stage < last)
    def _():
        attend(kvp_b, kvb, mask_b, seq_b, h_b)
        project(second, h_b, xin_b, x1buf.at[:, part_b, :])
        rms_into(x1buf.at[:, part_b, :], 1, h_b)
        gate_up(second, h_b, abuf.at[:, part_b, :], False)
        @pl.when(stage == 0)
        def _():
            down(abuf.at[:, part_b, :], x1buf.at[:, part_b, :], xout_b, 1, False)

        @pl.when(stage > 0)
        def _():
            down(abuf.at[:, part_b, :], x1buf.at[:, part_b, :], xout_b, 1, True)

        emit_a()
        emit_b()

    def res_copy(d, src_col):
        return pltpu.make_async_remote_copy(src_ref=res_vm, dst_ref=res_out.at[src_col], send_sem=rs_sem.at[d], recv_sem=rr_sem.at[src_col],
                                            device_id=device(d), device_id_type=MESH)

    def res_local():
        return pltpu.make_async_copy(res_vm, res_out.at[col], rs_sem.at[me])

    groups = n_dec // 4

    @pl.when(stage == last)
    def _():
        xs, hs, qs, x1s, ys = (small.at[i] for i in range(5))
        off_b = len_b - 1 - half * seq_b

        def one_hot(rows, first, last_row, dec_row, dec_on):
            who = lax.broadcasted_iota(jnp.int32, (n_dec, rows), 0)
            at = lax.broadcasted_iota(jnp.int32, (n_dec, rows), 1)
            hit = ((who == first) & (at < dec_row) & (at == last_row)) | ((who == first + 2) & dec_on & (at == dec_row))
            return jnp.where(hit, 1.0, 0.0).astype(bf)

        sel_a = one_hot(rows_a, 0, len_a - 1, seq_a, stage == last)
        sel_b = one_hot(rows_b, 1, off_b, seq_b, half == 1)
        for n in range(nl // 2):
            for src_a, src_b, dst in ((xin_a, xin_b, xs), (h_a, h_b, hs)):
                y = (dot_nn(sel_a, cat(src_a, 2 * n, 2)) + dot_nn(sel_b, cat(src_b, 2 * n, 2))).astype(bf)
                dst[2 * n] = y[:, :LANES]
                dst[2 * n + 1] = y[:, LANES:]
        queries(0, hs, qs, tsmall.at[0], tsmall.at[1])
        emit_b()

        stack = pairs_per_kv * n_dec
        key = lax.broadcasted_iota(jnp.int32, (stack, LANES), 1)
        row = lax.rem(lax.broadcasted_iota(jnp.int32, (stack, LANES), 0), n_dec)
        low_k = key < head_dim
        mk_a, mk_b = (key < len_a).astype(f32), (key < len_b).astype(f32)
        decode = (row[:, 0:1] == 2) | (row[:, 0:1] == 3)
        from_a = lax.rem(row, 2) == 0
        for c in range(kv_heads):
            kd = kvd[c].astype(f32)
            kr = pltpu.roll(kd, head_dim, 1)
            k_two, v_two = jnp.where(low_d, kd, kr), jnp.where(low_d, kr, kd)
            k_self = jnp.where(from_a, k_two[0:1], k_two[1:2])
            v_self = jnp.where(from_a, v_two[0:1], v_two[1:2])
            q4 = jnp.concatenate([qs[c * pairs_per_kv + t] for t in range(pairs_per_kv)], axis=0)
            prod = q4.astype(f32) * k_self
            self_e = jnp.where(decode, jnp.sum(jnp.where(low_k, prod, 0.0), axis=-1, keepdims=True) * scale, NEG)
            self_o = jnp.where(decode, jnp.sum(jnp.where(low_k, 0.0, prod), axis=-1, keepdims=True) * scale, NEG)
            outs = []
            for kv, mk in ((kva, mk_a), (kvb, mk_b)):
                sc = dot_nt(q4, kv[c, 0])
                pe, pe_s = soft_self(sc[:, :seq_a], mk, self_e)
                po, po_s = soft_self(sc[:, seq_a:], mk, self_o)
                outs.append(dot_nn(jnp.concatenate([pe, po], axis=1), kv[c, 1]) + jnp.where(low_k, pe_s, po_s) * v_self)
            o = jnp.where(from_a, outs[0], outs[1]).astype(bf)
            for t in range(pairs_per_kv):
                hs[c * pairs_per_kv + t] = o[t * n_dec:(t + 1) * n_dec]

        project(0, hs, xs, x1s)
        rms_into(x1s, 1, hs)
        gate_up(0, hs, asmall, False)
        down(asmall, x1s, ys, None, True)
        keep = (row_d == 0) | (row_d == 2) | ((row_d == 1) & (off_b >= 0) & (off_b < seq_b)) | ((row_d == 3) & (half == 1))
        for n in range(2 * nx // groups):
            j, p = n // 2, n % 2
            acc = jnp.zeros((n_dec, LANES), f32)
            for i in range(groups):
                y = jnp.where(keep, ys[2 * (groups * j + i) + p].astype(f32), 0.0)
                y = pltpu.roll(y, 4 * i, 0) if i else y
                acc = jnp.where(row_d // 4 == i, y, acc)
            res_vm[:, n * LANES:(n + 1) * LANES] = acc.astype(bf)
        others(lambda d: res_copy(d, col).start())
        res_local().start()
        others(lambda d: res_copy(d, col).wait_send())
        res_local().wait()

    @pl.when(stage < last)
    def _():
        for k in range(2):
            for n in range(nx):
                x_send(k, n).wait_send()

    @pl.when(half == 0)
    def _():
        pair_copy().wait_send()

    others(lambda d: dec_copy(d, stage, col).wait_send())
    dec_local().wait()
    others(lambda d: kv_copy(d, 0, stage, col).wait_send())
    kv_local(0, col).wait()

    @pl.when(half == 1)
    def _():
        others(lambda d: kv_copy(d, 1, stage, shared).wait_send())
        kv_local(1, shared).wait()

    others(lambda d: dec_copy(0, d // width, lax.rem(d, width)).wait_recv())
    for b in range(n_prompts):
        owner = b if b < width else 2 * (b - width) + 1

        def kv_in(s, carry, b=b, owner=owner):
            @pl.when((s != stage) | (col != owner))
            def _():
                kv_copy(0, 0, s, b).wait_recv()
            return carry

        lax.fori_loop(0, stages, kv_in, 0)

    def res_in(y, carry):
        @pl.when((stage != last) | (y != col))
        def _():
            res_copy(0, y).wait_recv()
        return carry

    lax.fori_loop(0, width, res_in, 0)


def solution(mesh):
    stages = mesh.shape['model']
    width = mesh.shape['model2']
    stage_spec = P('model', None, None)
    in_specs = (P('replica', None, None, None), P('replica', None), P('replica', None),
                stage_spec, stage_spec, stage_spec, stage_spec, P(None, None), P(None, None),
                P(None, None, TP_AXES, None), P(None, None, TP_AXES, None), P(None, None, TP_AXES, None),
                P(None, TP_AXES, None, None), P(None, None, TP_AXES), P(None, None, TP_AXES), P(None, TP_AXES, None))
    cache_spec = P(None, 'replica', None, TP_AXES, None)
    out_specs = (P('replica', None), P('replica', None), cache_spec, cache_spec)

    def shard_body(x_prompt, lengths, x_new, st_qkv, st_out, st_gateup, st_down_t, gain_attn, gain_mlp, tp_query, tp_key, tp_value, tp_out, tp_gate, tp_up, tp_down):
        n_prompts, _, seq_len, d_model = x_prompt.shape
        head_dim = tp_query.shape[-1]
        q_cols = st_out.shape[1]
        kv_heads = (st_qkv.shape[2] - q_cols) // (2 * head_dim)
        ff = st_down_t.shape[2]
        n_dec = 16
        seq_a, seq_b = seq_len, seq_len // 2
        assert n_prompts == width + width // 2 and st_qkv.shape[0] == 1 and tp_key.shape[2] == 1
        rows_a, rows_b = seq_a + n_dec, seq_b + n_dec
        groups = n_dec // 4
        bf, f32 = jnp.bfloat16, jnp.float32
        cos_t, sin_t = rope_table(seq_len + 8, head_dim)
        dims = (stages, width, kv_heads, head_dim, seq_a, seq_b, n_dec, q_cols, ff, n_prompts)
        nx, nl = d_model // BLK, d_model // LANES
        n_dev = stages * width
        vmem, hbm = pl.BlockSpec(memory_space=pltpu.VMEM), pl.BlockSpec(memory_space=pl.ANY)
        smem = pl.BlockSpec(memory_space=pltpu.SMEM)
        dma = pltpu.SemaphoreType.DMA
        kv_all, dec_all, res = pl.pallas_call(
            functools.partial(stage_kernel, dims),
            out_shape=(jax.ShapeDtypeStruct((stages, n_prompts, 2, head_dim, seq_len), bf), jax.ShapeDtypeStruct((stages, width, n_dec, LANES), bf), jax.ShapeDtypeStruct((width, n_dec, d_model // groups), bf)),
            in_specs=[smem] + [vmem] * 5 + [hbm] * 5,
            out_specs=(hbm, hbm, hbm),
            scratch_shapes=[
                pltpu.VMEM((2 * NSLOT, d_model, LANES), bf),
                pltpu.VMEM((ff // LANES, d_model, LANES), bf),
                pltpu.VMEM((nl, rows_a, LANES), bf),
                pltpu.VMEM((nl, rows_b, LANES), bf),
                pltpu.VMEM((nl, rows_a, LANES), bf),
                pltpu.VMEM((nl, rows_b, LANES), bf),
                pltpu.VMEM((nl, rows_a, LANES), bf),
                pltpu.VMEM((nl, rows_b, LANES), bf),
                pltpu.VMEM((q_cols // LANES, rows_a, LANES), bf),
                pltpu.VMEM((nl, rows_a, LANES), bf),
                pltpu.VMEM((ff // LANES, rows_a, LANES), bf),
                pltpu.VMEM((kv_heads, rows_a, LANES), bf),
                pltpu.VMEM((kv_heads, rows_b, LANES), bf),
                pltpu.VMEM((kv_heads, 2, 2 * seq_a, LANES), bf),
                pltpu.VMEM((kv_heads, 3, 2 * seq_a, LANES), bf),
                pltpu.VMEM((kv_heads, seq_b, LANES), bf),
                pltpu.VMEM((kv_heads, 2, 2, head_dim, seq_len), bf),
                pltpu.VMEM((kv_heads, n_dec, LANES), bf),
                pltpu.VMEM((2, rows_a, LANES), f32),
                pltpu.VMEM((2, rows_b, LANES), f32),
                pltpu.VMEM((2, nl, 8, LANES), f32),
                pltpu.VMEM((rows_a, LANES), f32),
                pltpu.VMEM((rows_b, LANES), f32),
                pltpu.VMEM((n_dec, d_model // groups), bf),
                pltpu.VMEM((5, nl, n_dec, LANES), bf),
                pltpu.VMEM((ff // LANES, n_dec, LANES), bf),
                pltpu.VMEM((2, n_dec, LANES), f32),
                dma((2 * NSLOT,)), dma((ff // LANES,)), dma((2 * nl,)), dma((2, nx)), dma((2, nx)), dma((3, n_dev)), dma((stages * n_prompts,)), dma((n_dev,)), dma((n_dev,)), dma((width,)), dma((2,)),
            ],
            compiler_params=pltpu.CompilerParams(collective_id=0, has_side_effects=True, vmem_limit_bytes=67043328),
        )(lengths, cos_t, sin_t, gain_attn, gain_mlp, x_new, x_prompt, st_qkv, st_out, st_gateup, st_down_t)

        picked = res.reshape(width, groups, 4, nx // groups, BLK).transpose(0, 2, 3, 1, 4).reshape(width, 4, d_model)
        last_hidden = jnp.concatenate([picked[:, 0], picked[0::2, 1] + picked[1::2, 1]], axis=0)
        dec_out = jnp.concatenate([picked[:, 2], picked[1::2, 3]], axis=0)

        dec_kv = jnp.concatenate([dec_all[:, :, 0], dec_all[:, 1::2, 1]], axis=1)

        def cache(part):
            own = dec_kv[:, :, part * head_dim:(part + 1) * head_dim]
            return jnp.concatenate([kv_all[:, :, part], own[..., None]], axis=3).transpose(0, 1, 3, 2)[:, :, :, None, :]

        return dec_out, last_hidden, cache(0), cache(1)

    return jax.shard_map(shard_body, mesh=mesh, in_specs=in_specs, out_specs=out_specs, check_vma=False)
```
